128 devices in a mesh: ctx: 16 (over y, x), tp: 8 (over z, core).
Axes of the slice: x: 4, y: 4, z: 4, core: 2. Of those that a mesh axis runs over, the one named last changes fastest.
Arguments:
- hidden: bfloat16 [8, 8192], P(None, 'ctx'), may hold values from -4.8 to 4.8, as said below
- norm_gains: bfloat16 [4, 8192], P(None, 'ctx'), may hold values from 0.5 to 1.5
- w_query: bfloat16 [4, 8192, 8192], P(None, 'ctx', 'tp'), may hold values from -0.0625 to 0.0625
- w_key: bfloat16 [4, 8192, 1024], P(None, 'ctx', 'tp'), may hold values from -0.125 to 0.125
- w_value: bfloat16 [4, 8192, 1024], P(None, 'ctx', 'tp'), may hold values from -0.125 to 0.125
- w_out: bfloat16 [4, 8192, 8192], P(None, 'tp', 'ctx'), may hold values from -0.0625 to 0.0625
- key_cache: bfloat16 [4, 8, 8, 2048, 128], P(None, None, 'tp', 'ctx'), may hold values from -9 to 9
- value_cache: bfloat16 [4, 8, 8, 2048, 128], P(None, None, 'tp', 'ctx'), may hold values from -6 to 6
- lengths: int32 [8], replicated, may hold values from 1 to 2048, 8200 in all
Outputs:
- updated: float32 [8, 8192], P(None, 'ctx')
The draws below stay inside these ranges and needn't reach their ends.
Inputs may be any that keep to these rules, and one draw needn't show every extreme that they name: Each sequence has lengths[b] valid cache positions 0 .. lengths[b] - 1, between 1 and 2048; the longest sequence has exactly 2048; the new token sits at position lengths[b]. `hidden`: activations of order 0.2; in each block of 512 consecutive features one sequence, chosen at random, has entries four times larger.
All inputs are finite; a program needn't handle non-finite values.
Results may differ from the reference program's by a relative error of at most 0.02.
Values sent between devices are 32-bit elements.
A program may use at most 64 MiB of HBM per device.

```python
import math
import jax
import jax.numpy as jnp
import numpy as np
from jax import lax

D = 8192
HQ = 64
KVH = 8
HD = 128
LAYERS = 4
BATCH = 8
CAP = 2048
D_DEV = 512


def draw_hidden(key, part):
    base_key, owner_key = jax.random.split(jax.random.fold_in(key, 7))
    block_count = D // D_DEV
    owners = jax.random.randint(owner_key, (block_count,), 0, BATCH)
    column_owner = owners[jnp.arange(D) // D_DEV]
    factor = jnp.where(column_owner[None, :] == jnp.arange(BATCH)[:, None], 4.0, 1.0)
    base_draw = jnp.clip(jax.random.normal(base_key, (BATCH, D), jnp.float32), -6.0, 6.0)
    return (0.2 * factor * base_draw).astype(jnp.bfloat16)


def block_scale(rng, extent, pieces, smallest, high):
    gain = 1.0
    for axis_at, parts in pieces:
        draws = jax.random.uniform(jax.random.fold_in(jax.random.fold_in(rng, 6), axis_at), (parts,), jnp.float32, smallest / len(pieces), high / len(pieces))
        gain = gain * jnp.repeat(jnp.exp(draws), extent[axis_at] // parts).reshape((-1,) + (1,) * (len(extent) - 1 - axis_at))
    return gain


def profile(count, total, reach, slope):
    portions = [(1 << 20) // math.isqrt(grade ** slope) + 1 for grade in range(2, count + 1)]
    surplus, given = total - reach - (count - 1), [1] * (count - 1)
    while surplus > 0:
        movable = [i for i in range(count - 1) if given[i] < reach]
        mass, remaining = sum([portions[i] for i in movable]), surplus
        for i in movable:
            extra = min(reach - given[i], max(1, remaining * portions[i] // mass), surplus)
            given[i] = given[i] + extra
            surplus = surplus - extra
    return np.array([reach] + given)


def ragged(rng, amount, total, most, lean):
    if amount == 2:
        one = jax.random.randint(rng, (), max(1, total - most), min(most, total - 1) + 1)
        return jnp.stack([one, total - one])
    sizes = jnp.asarray(profile(amount, total, most, lean), jnp.int32)
    couples = (amount - 1) // 2
    source_of, taker = sizes[1:1 + 2 * couples:2], sizes[2:2 + 2 * couples:2]
    slack = jnp.minimum(source_of - 1, most - taker)
    shifted = jax.random.randint(jax.random.fold_in(rng, 1), (couples,), 0, 1 << 20) % (slack + 1)
    sizes = sizes.at[1:1 + 2 * couples:2].set(source_of - shifted).at[2:2 + 2 * couples:2].set(taker + shifted)
    return sizes[jax.random.permutation(jax.random.fold_in(rng, 2), amount)]


def scatter_about(stream_key, dims, scale, limit, pieces=(), kind=jnp.bfloat16):
    array = scale * jax.random.normal(stream_key, dims, jnp.float32)
    if pieces:
        array = array * block_scale(stream_key, dims, pieces, -0.22, 0.18)
    return jnp.clip(array, -limit, limit).astype(kind)


def setup_inputs(seed: int = 0) -> dict:
    key_list = jax.random.split(jax.random.key(seed), 10)
    hidden = draw_hidden(jax.random.fold_in(key_list[9], 71), 0)
    norm_gains = jnp.clip(1.0 + 0.1 * jax.random.normal(key_list[1], (LAYERS, D), jnp.float32), 0.5, 1.5).astype(jnp.bfloat16)
    w_query = scatter_about(key_list[2], (LAYERS, D, HQ * HD), D ** -0.5, 0.0625, ((1, 16), (2, 8)))
    w_key = scatter_about(key_list[3], (LAYERS, D, KVH * HD), (D // 4) ** -0.5, 0.125, ((1, 16), (2, 8)))
    w_value = scatter_about(key_list[4], (LAYERS, D, KVH * HD), (D // 4) ** -0.5, 0.125, ((1, 16), (2, 8)))
    w_out = scatter_about(key_list[5], (LAYERS, HQ * HD, D), (HQ * HD) ** -0.5, 0.0625, ((1, 8), (2, 16)))
    key_cache = scatter_about(key_list[6], (LAYERS, BATCH, KVH, CAP, HD), 1.5, 9.0, ((2, 8), (3, 16)))
    value_cache = scatter_about(key_list[7], (LAYERS, BATCH, KVH, CAP, HD), 1.0, 6.0, ((2, 8), (3, 16)))
    lengths = ragged(key_list[8], BATCH, BATCH * CAP // 2 + BATCH, CAP, 2).astype(jnp.int32)
    return dict(hidden=hidden, norm_gains=norm_gains, w_query=w_query, w_key=w_key, w_value=w_value, w_out=w_out, key_cache=key_cache, value_cache=value_cache, lengths=lengths)


mask_fill = -1e+30
norm_eps = 1e-05
rope_base = 500000.0

def rotate(vectors, positions):
    width = vectors.shape[-1]
    half_width = width // 2
    exponents = jnp.arange(half_width, dtype=jnp.float32) * (2.0 / width)
    frequency = jnp.exp(-exponents * math.log(rope_base))
    angles = positions.astype(jnp.float32)[:, None] * frequency[None, :]
    cosine = jnp.cos(angles)[:, None, :]
    sine_part = jnp.sin(angles)[:, None, :]
    first_half = vectors[..., :half_width]
    second_half = vectors[..., half_width:]
    return jnp.concatenate([first_half * cosine - second_half * sine_part, second_half * cosine + first_half * sine_part], axis=-1)

def reference(hidden, norm_gains, w_query, w_key, w_value, w_out, key_cache, value_cache, lengths):
    stream = hidden.astype(jnp.float32)
    group_size = HQ // KVH
    logit_multiplier = 1.0 / math.sqrt(HD)
    positions = jnp.arange(CAP, dtype=jnp.int32)
    usable = (positions[None, :] < lengths[:, None])[:, None, None, :]
    for layer_idx in range(LAYERS):
        reciprocal_value = lax.rsqrt(lax.optimization_barrier(jnp.sum(stream * stream, axis=1)) / D + norm_eps)
        scaled = (stream * norm_gains[layer_idx].astype(jnp.float32)).astype(jnp.bfloat16)
        raw_query = jnp.dot(scaled, w_query[layer_idx], preferred_element_type=jnp.float32)
        raw_key = jnp.dot(scaled, w_key[layer_idx], preferred_element_type=jnp.float32)
        raw_value = jnp.dot(scaled, w_value[layer_idx], preferred_element_type=jnp.float32)
        query = rotate((raw_query * reciprocal_value[:, None]).reshape(BATCH, HQ, HD), lengths).astype(jnp.bfloat16)
        fresh_lookup_vector = rotate((raw_key * reciprocal_value[:, None]).reshape(BATCH, KVH, HD), lengths).astype(jnp.bfloat16)
        new_value = (raw_value * reciprocal_value[:, None]).reshape(BATCH, KVH, HD).astype(jnp.bfloat16)
        shared_head_sets = query.reshape(BATCH, KVH, group_size, HD).astype(jnp.float32)
        scores = jnp.einsum('bkgd,bksd->bkgs', shared_head_sets, key_cache[layer_idx].astype(jnp.float32), precision=lax.Precision.HIGHEST) * logit_multiplier
        self_match_logit = jnp.einsum('uryj,urj->ury', shared_head_sets, fresh_lookup_vector.astype(jnp.float32), precision=lax.Precision.HIGHEST) * logit_multiplier
        masked = jnp.where(usable, scores, mask_fill)
        largest = jnp.maximum(lax.optimization_barrier(jnp.max(masked, axis=-1)), self_match_logit)
        attention_probabilities = jnp.where(usable, jnp.exp(masked - largest[..., None]), 0.0)
        fresh = jnp.exp(self_match_logit - largest)
        nearest_whole = lax.optimization_barrier(attention_probabilities.astype(jnp.bfloat16)).astype(jnp.float32)
        fresh_rounded = lax.optimization_barrier(fresh.astype(jnp.bfloat16)).astype(jnp.float32)
        numerator = jnp.einsum('bkgs,bksd->bkgd', nearest_whole, value_cache[layer_idx].astype(jnp.float32), precision=lax.Precision.HIGHEST)
        numerator = numerator + fresh_rounded[..., None] * new_value.astype(jnp.float32)[:, :, None, :]
        denominator = lax.optimization_barrier(jnp.sum(attention_probabilities, axis=-1)) + fresh
        context = (numerator / denominator[..., None]).reshape(BATCH, HQ * HD).astype(jnp.bfloat16)
        stream = stream + jnp.dot(context, w_out[layer_idx], preferred_element_type=jnp.float32)
    return stream
```

```python
import functools
import math

import jax
import jax.numpy as jnp
from jax import lax
from jax.experimental import pallas as pl
from jax.experimental.pallas import tpu as pltpu
from jax.sharding import Mesh
from jax.sharding import PartitionSpec as P

CTX = ("ctx_0", "ctx_1")
MESH = pl.DeviceIdType.MESH
NORM_EPS = 1e-05
ROPE_BASE = 500000.0
MASK_FILL = -1e30
RING = 4
FAR_FIRST = (2, 1, 3)
TP_STEPS = ((2, 0), (2, 1), (1, 0), (1, 1), (3, 0), (3, 1), (0, 1))
FIRST = 768


def kernel(
    layers, batch, heads, width, span, features,
    hidden_hbm, gains_hbm, wq_hbm, wk_hbm, wv_hbm, wo_hbm, kc_hbm, vc_hbm, lengths,
    out_ref,
    hidden_v, gains_v, wqkv, wo, kcat, vcat, diag,
    a1x, a1y, a2y, a2x, b1x, b1y, b2y, b2x, cbuf,
    in_sem, w_sem, a_send, a_recv, c_send, c_recv,
):
    y = lax.axis_index("ctx_0")
    x = lax.axis_index("ctx_1")
    tp = lax.axis_index("tp")
    z, core = tp // 2, lax.rem(tp, 2)
    columns = heads * width
    f32, bf16 = jnp.float32, jnp.bfloat16

    def tp_partner(step, sign=1):
        dz, other = step
        zz = lax.rem(z + (dz if sign > 0 else RING - dz), RING)
        cc = 1 - core if other else core
        return zz * 2 + cc

    barrier = pltpu.get_barrier_semaphore()
    for d in FAR_FIRST:
        pl.semaphore_signal(barrier, inc=1, device_id={"ctx_1": lax.rem(x + d, RING)}, device_id_type=MESH)
        pl.semaphore_signal(barrier, inc=1, device_id={"ctx_0": lax.rem(y + d, RING)}, device_id_type=MESH)
    for step in TP_STEPS:
        pl.semaphore_signal(barrier, inc=1, device_id={"tp": tp_partner(step)}, device_id_type=MESH)

    def weight_copies(l):
        return (
            pltpu.make_async_copy(wq_hbm.at[l], wqkv.at[l, :, pl.ds(0, columns)], w_sem.at[l, 0]),
            pltpu.make_async_copy(wk_hbm.at[l], wqkv.at[l, :, pl.ds(columns, width)], w_sem.at[l, 1]),
            pltpu.make_async_copy(wv_hbm.at[l], wqkv.at[l, :, pl.ds(columns + width, width)], w_sem.at[l, 2]),
        )

    def late_start(l):
        for b in range(batch):
            pltpu.make_async_copy(
                kc_hbm.at[l, b], kcat.at[l, :, pl.ds(b * width, width)], w_sem.at[l, 3]
            ).start()
        pltpu.make_async_copy(vc_hbm.at[l], vcat.at[l], w_sem.at[l, 4]).start()
        pltpu.make_async_copy(wo_hbm.at[l], wo.at[l], w_sem.at[l, 5]).start()

    hidden_copy = pltpu.make_async_copy(hidden_hbm, hidden_v, in_sem.at[0])
    gains_copy = pltpu.make_async_copy(gains_hbm, gains_v, in_sem.at[1])
    hidden_copy.start()
    gains_copy.start()
    for copy in weight_copies(0):
        copy.start()
    late_start(0)
    for l in range(1, layers):
        for copy in weight_copies(l):
            copy.start()
        late_start(l)

    row = lax.broadcasted_iota(jnp.int32, (batch, width), 0)
    lane = lax.broadcasted_iota(jnp.int32, (batch, width), 1)
    half = width // 2
    length = jnp.zeros((batch, width), jnp.int32)
    for b in range(batch):
        length = jnp.where(row == b, lengths[b], length)
    low = lane < half
    exponents = jnp.where(low, lane, lane - half).astype(f32) * (2.0 / width)
    angles = length.astype(f32) * jnp.exp(-exponents * math.log(ROPE_BASE))
    cosine = jnp.cos(angles)
    sine = jnp.where(low, -jnp.sin(angles), jnp.sin(angles))
    usable = (y * RING + x) * span + lane < length
    scale = 1.0 / math.sqrt(width)
    wide_row = lax.broadcasted_iota(jnp.int32, (2 * batch, batch * width), 0)
    wide_col = lax.broadcasted_iota(jnp.int32, (2 * batch, batch * width), 1)
    own_block = jnp.where(lax.rem(wide_row, batch) == wide_col // width, 1.0, 0.0).astype(bf16)
    for part in range(heads // 2):
        diag[pl.ds(part * 2 * batch, 2 * batch), :] = own_block

    def rotate(u):
        return u * cosine + pltpu.roll(u, half, axis=1) * sine

    def spread(tall):
        return jnp.concatenate([tall] * batch, axis=1) * diag[...]

    def ring_copy(buf, l, axis, me, phase, d):
        return pltpu.make_async_remote_copy(
            src_ref=buf.at[l, me], dst_ref=buf.at[l, me],
            send_sem=a_send.at[l, phase, d - 1], recv_sem=a_recv.at[l, phase, d - 1],
            device_id={axis: lax.rem(me + d, RING)}, device_id_type=MESH,
        )

    def ring_start(*args):
        for d in FAR_FIRST:
            ring_copy(*args, d).start()

    def ring_arrive(buf, l, axis, me, phase):
        for d in (1, 3, 2):
            ring_copy(buf, l, axis, me, phase, d).wait_recv()

    def ring_sent(*args):
        for d in FAR_FIRST:
            ring_copy(*args, d).wait_send()

    def tp_copy(l, k):
        return pltpu.make_async_remote_copy(
            src_ref=cbuf.at[l, tp], dst_ref=cbuf.at[l, tp],
            send_sem=c_send.at[l, k], recv_sem=c_recv.at[l, k],
            device_id={"tp": tp_partner(TP_STEPS[k])}, device_id_type=MESH,
        )

    def total(buf, l):
        return (buf[l, 0] + buf[l, 1]) + (buf[l, 2] + buf[l, 3])

    def tile(values, i):
        return values[:, i * width:(i + 1) * width]

    def over_lane(values, i):
        return jnp.broadcast_to(values[:, i:i + 1], (batch, width))

    def merge(buf, l):
        group = heads // 2
        stats = [buf[l, s, :, pl.ds(group * width, width)] for s in range(RING)]
        top = functools.reduce(jnp.maximum, stats)
        shrink = [jnp.exp(t - top) for t in stats]
        sums = functools.reduce(
            jnp.add, [pltpu.roll(e, half, axis=1) * t for e, t in zip(shrink, stats)]
        )
        out = []
        for i in range(group):
            parts = [
                over_lane(shrink[s], i) * buf[l, s, :, pl.ds(i * width, width)] for s in range(RING)
            ]
            out.append((parts[0] + parts[1]) + (parts[2] + parts[3]))
        return out, jnp.where(low, top, sums)

    def finish(buf, l, own, new_value):
        group = heads // 2
        stats = [buf[l, s, :, pl.ds(group * width, width)] for s in range(RING)] + [own]
        top = functools.reduce(jnp.maximum, stats)
        shrink = [jnp.exp(t - top) for t in stats]
        sums = functools.reduce(
            jnp.add, [e * pltpu.roll(t, half, axis=1) for e, t in zip(shrink, stats)]
        )
        share = [e / sums for e in shrink]
        out = []
        for i in range(group):
            parts = [
                over_lane(share[s], i) * buf[l, s, :, pl.ds(i * width, width)] for s in range(RING)
            ] + [over_lane(share[RING], i) * new_value]
            out.append((parts[0] + parts[1]) + (parts[2] + parts[3]) + parts[4])
        return out

    hidden_copy.wait()
    gains_copy.wait()

    def layer(l, stream):
        for copy in weight_copies(l):
            copy.wait()
        gain = gains_v[pl.ds(l, 1), :].astype(f32)
        scaled = (stream * gain).astype(bf16)
        a1x[l, x] = jnp.dot(scaled, wqkv[l, :, pl.ds(0, FIRST)], preferred_element_type=f32)
        if isinstance(l, int) and l == 0:
            pl.semaphore_wait(barrier, 2 * (RING - 1) + len(TP_STEPS))
        ring_start(a1x, l, "ctx_1", x, 0)
        rest = columns + 2 * width - FIRST
        a1y[l, y, :, pl.ds(0, rest)] = jnp.dot(
            scaled, wqkv[l, :, pl.ds(FIRST, rest)], preferred_element_type=f32
        )
        squares = stream * stream
        a1y[l, y, :, pl.ds(rest, width)] = functools.reduce(
            jnp.add, [tile(squares, i) for i in range(features // width)]
        )
        ring_start(a1y, l, "ctx_0", y, 1)

        ring_arrive(a1x, l, "ctx_1", x, 0)
        a2y[l, y] = total(a1x, l)
        ring_start(a2y, l, "ctx_0", y, 2)
        ring_arrive(a1y, l, "ctx_0", y, 1)
        a2x[l, x] = total(a1y, l)
        ring_start(a2x, l, "ctx_1", x, 3)
        ring_arrive(a2y, l, "ctx_0", y, 2)
        ring_arrive(a2x, l, "ctx_1", x, 3)

        raw = jnp.concatenate([total(a2y, l), total(a2x, l)], axis=1)
        mean = jnp.sum(tile(raw, heads + 2), axis=1, keepdims=True) / (RING * RING * features)
        inverse = lax.rsqrt(mean + NORM_EPS)
        query = [rotate(tile(raw, h) * inverse).astype(bf16) for h in range(heads)]
        tall = jnp.concatenate(query, axis=0)
        pltpu.make_async_copy(kcat.at[l], kcat.at[l], w_sem.at[l, 3]).wait()
        scores = lax.dot_general(
            spread(tall), kcat[l], (((1,), (1,)), ((), ())), preferred_element_type=f32
        ) * scale
        zero = jnp.zeros((batch, width), f32)
        stats_first, stats_last = zero, zero
        weights = []
        for h in range(heads):
            masked = jnp.where(usable, scores[h * batch:(h + 1) * batch], MASK_FILL)
            top = jnp.max(masked, axis=1, keepdims=True)
            weight = jnp.where(usable, jnp.exp(masked - top), 0.0)
            amount = jnp.sum(weight, axis=1, keepdims=True)
            weights.append(weight.astype(bf16))
            i = h % (heads // 2)
            if h < heads // 2:
                stats_first = jnp.where(lane == i, top, jnp.where(lane == half + i, amount, stats_first))
            else:
                stats_last = jnp.where(lane == i, top, jnp.where(lane == half + i, amount, stats_last))
        pltpu.make_async_copy(vc_hbm.at[l], vcat.at[l], w_sem.at[l, 4]).wait()
        sums = jnp.dot(
            spread(jnp.concatenate(weights, axis=0)), vcat[l], preferred_element_type=f32
        )
        group = heads // 2
        for i in range(group):
            b1x[l, x, :, pl.ds(i * width, width)] = sums[i * batch:(i + 1) * batch]
        b1x[l, x, :, pl.ds(group * width, width)] = stats_first
        ring_start(b1x, l, "ctx_1", x, 4)
        for i in range(group):
            b1y[l, y, :, pl.ds(i * width, width)] = sums[(group + i) * batch:(group + i + 1) * batch]
        b1y[l, y, :, pl.ds(group * width, width)] = stats_last
        ring_start(b1y, l, "ctx_0", y, 5)

        new_key = rotate(tile(raw, heads) * inverse).astype(bf16).astype(f32)
        new_value = (tile(raw, heads + 1) * inverse).astype(bf16).astype(f32)
        own = []
        for g in range(2):
            packed = jnp.where(lane >= half, 1.0, 0.0)
            for i in range(group):
                match = jnp.sum(query[g * group + i].astype(f32) * new_key, axis=1, keepdims=True)
                packed = jnp.where(lane == i, match * scale, packed)
            own.append(packed)
        ring_sent(a1x, l, "ctx_1", x, 0)
        ring_sent(a1y, l, "ctx_0", y, 1)
        ring_sent(a2y, l, "ctx_0", y, 2)
        ring_sent(a2x, l, "ctx_1", x, 3)

        ring_arrive(b1x, l, "ctx_1", x, 4)
        merged, stats = merge(b1x, l)
        for i in range(group):
            b2y[l, y, :, pl.ds(i * width, width)] = merged[i]
        b2y[l, y, :, pl.ds(group * width, width)] = stats
        ring_start(b2y, l, "ctx_0", y, 6)
        ring_arrive(b1y, l, "ctx_0", y, 5)
        merged, stats = merge(b1y, l)
        for i in range(group):
            b2x[l, x, :, pl.ds(i * width, width)] = merged[i]
        b2x[l, x, :, pl.ds(group * width, width)] = stats
        ring_start(b2x, l, "ctx_1", x, 7)
        pltpu.make_async_copy(wo_hbm.at[l], wo.at[l], w_sem.at[l, 5]).wait()
        ring_arrive(b2y, l, "ctx_0", y, 6)
        context = finish(b2y, l, own[0], new_value)
        ring_arrive(b2x, l, "ctx_1", x, 7)
        context = context + finish(b2x, l, own[1], new_value)
        context = jnp.concatenate(context, axis=1).astype(bf16)
        cbuf[l, tp] = jnp.dot(context, wo[l], preferred_element_type=f32)
        for k in range(len(TP_STEPS)):
            tp_copy(l, k).start()
        ring_sent(b1x, l, "ctx_1", x, 4)
        ring_sent(b1y, l, "ctx_0", y, 5)
        ring_sent(b2y, l, "ctx_0", y, 6)
        ring_sent(b2x, l, "ctx_1", x, 7)
        for k in reversed(range(len(TP_STEPS))):
            tp_copy(l, k).wait_recv()
        parts = [cbuf[l, t] for t in range(2 * RING)]
        stream = stream + (
            ((parts[0] + parts[1]) + (parts[2] + parts[3])) + ((parts[4] + parts[5]) + (parts[6] + parts[7]))
        )
        for k in range(len(TP_STEPS)):
            tp_copy(l, k).wait_send()
        return stream

    stream = hidden_v[...].astype(f32)
    for l in range(layers):
        stream = layer(l, stream)
    out_ref[...] = stream


def on_device(hidden, norm_gains, w_query, w_key, w_value, w_out, key_cache, value_cache, lengths):
    layers, features, columns = w_query.shape
    batch, _, span, width = key_cache.shape[1:]
    heads = columns // width
    keys = key_cache.reshape(layers, batch, span, width)
    values = value_cache.reshape(layers, batch * span, width)
    f32, bf16 = jnp.float32, jnp.bfloat16
    total = columns + 2 * width
    last = total - FIRST + width
    packed = (heads // 2 + 1) * width
    anywhere = pl.BlockSpec(memory_space=pl.ANY)
    return pl.pallas_call(
        functools.partial(kernel, layers, batch, heads, width, span, features),
        out_shape=jax.ShapeDtypeStruct((batch, features), f32),
        in_specs=[anywhere] * 8 + [pl.BlockSpec(memory_space=pltpu.SMEM)],
        out_specs=pl.BlockSpec(memory_space=pltpu.VMEM),
        scratch_shapes=[
            pltpu.VMEM((batch, features), bf16),
            pltpu.VMEM((layers, features), bf16),
            pltpu.VMEM((layers, features, total), bf16),
            pltpu.VMEM((layers, columns, features), bf16),
            pltpu.VMEM((layers, span, batch * width), bf16),
            pltpu.VMEM((layers, batch * span, width), bf16),
            pltpu.VMEM((heads * batch, batch * width), bf16),
            pltpu.VMEM((layers, RING, batch, FIRST), f32),
            pltpu.VMEM((layers, RING, batch, last), f32),
            pltpu.VMEM((layers, RING, batch, FIRST), f32),
            pltpu.VMEM((layers, RING, batch, last), f32),
            pltpu.VMEM((layers, RING, batch, packed), f32),
            pltpu.VMEM((layers, RING, batch, packed), f32),
            pltpu.VMEM((layers, RING, batch, packed), f32),
            pltpu.VMEM((layers, RING, batch, packed), f32),
            pltpu.VMEM((layers, 2 * RING, batch, features), f32),
            pltpu.SemaphoreType.DMA((2,)),
            pltpu.SemaphoreType.DMA((layers, 6)),
            pltpu.SemaphoreType.DMA((layers, 8, RING - 1)),
            pltpu.SemaphoreType.DMA((layers, 8, RING - 1)),
            pltpu.SemaphoreType.DMA((layers, len(TP_STEPS))),
            pltpu.SemaphoreType.DMA((layers, len(TP_STEPS))),
        ],
        compiler_params=pltpu.CompilerParams(
            collective_id=0, has_side_effects=True, vmem_limit_bytes=48 * 1024 * 1024
        ),
    )(hidden, norm_gains, w_query, w_key, w_value, w_out, keys, values, lengths)


def solution(mesh):
    finer = Mesh(mesh.devices.reshape(RING, RING, mesh.shape["tp"]), CTX + ("tp",))
    return jax.shard_map(
        on_device,
        mesh=finer,
        in_specs=(
            P(None, CTX),
            P(None, CTX),
            P(None, CTX, "tp"),
            P(None, CTX, "tp"),
            P(None, CTX, "tp"),
            P(None, "tp", CTX),
            P(None, None, "tp", CTX, None),
            P(None, None, "tp", CTX, None),
            P(),
        ),
        out_specs=P(None, CTX),
        check_vma=False,
    )
```

```python
import functools
import math

import jax
import jax.numpy as jnp
from jax import lax
from jax.experimental import pallas as pl
from jax.experimental.pallas import tpu as pltpu
from jax.sharding import Mesh
from jax.sharding import PartitionSpec as P

CTX = ("ctx_0", "ctx_1")
MESH = pl.DeviceIdType.MESH
NORM_EPS = 1e-05
ROPE_BASE = 500000.0
MASK_FILL = -1e30
RING = 4
FAR_FIRST = (2, 1, 3, 0)
TP_STEPS = ((2, 0), (2, 1), (1, 0), (1, 1), (3, 0), (3, 1), (0, 1))
FIRST = 768


def kernel(
    layers, batch, heads, width, span, features,
    hidden_hbm, gains_hbm, wq_hbm, wk_hbm, wv_hbm, wo_hbm, kc_hbm, vc_hbm, lengths_hbm,
    out_ref,
    lengths, hidden_v, gains_v, wqkv, wo, kcat, vcat, diag,
    a1x, a1y, a2y, a2x, b1x, b1y, b2y, b2x,
    a1xo, a1yo, a2yo, a2xo, b1xo, b1yo, b2yo, b2xo, cbuf,
    in_sem, w_sem, a_send, a_recv, c_send, c_recv,
):
    y = lax.axis_index("ctx_0")
    x = lax.axis_index("ctx_1")
    tp = lax.axis_index("tp")
    z, core = tp // 2, lax.rem(tp, 2)
    columns = heads * width
    f32, bf16 = jnp.float32, jnp.bfloat16

    def tp_partner(step, sign=1):
        dz, other = step
        zz = lax.rem(z + (dz if sign > 0 else RING - dz), RING)
        cc = 1 - core if other else core
        return zz * 2 + cc

    barrier = pltpu.get_barrier_semaphore()
    swapped = tp + 1 - 2 * core
    for d in FAR_FIRST[:-1]:
        pl.semaphore_signal(
            barrier, inc=1, device_id={"ctx_1": lax.rem(x + d, RING), "tp": swapped}, device_id_type=MESH
        )
        pl.semaphore_signal(
            barrier, inc=1, device_id={"ctx_0": lax.rem(y + d, RING), "tp": swapped}, device_id_type=MESH
        )
    for step in TP_STEPS:
        pl.semaphore_signal(barrier, inc=1, device_id={"tp": tp_partner(step)}, device_id_type=MESH)

    def weight_copies(l):
        return (
            pltpu.make_async_copy(wq_hbm.at[l], wqkv.at[l, :, pl.ds(0, columns)], w_sem.at[l, 0]),
            pltpu.make_async_copy(wk_hbm.at[l], wqkv.at[l, :, pl.ds(columns, width)], w_sem.at[l, 1]),
            pltpu.make_async_copy(wv_hbm.at[l], wqkv.at[l, :, pl.ds(columns + width, width)], w_sem.at[l, 2]),
        )

    def late_start(l):
        for b in range(batch):
            pltpu.make_async_copy(
                kc_hbm.at[l, b], kcat.at[l, :, pl.ds(b * width, width)], w_sem.at[l, 3]
            ).start()
        pltpu.make_async_copy(vc_hbm.at[l], vcat.at[l], w_sem.at[l, 4]).start()
        pltpu.make_async_copy(wo_hbm.at[l], wo.at[l], w_sem.at[l, 5]).start()

    hidden_copy = pltpu.make_async_copy(hidden_hbm, hidden_v, in_sem.at[0])
    gains_copy = pltpu.make_async_copy(gains_hbm, gains_v, in_sem.at[1])
    lengths_copy = pltpu.make_async_copy(lengths_hbm, lengths, in_sem.at[2])
    lengths_copy.start()
    hidden_copy.start()
    gains_copy.start()
    for copy in weight_copies(0):
        copy.start()

    lengths_copy.wait()
    row = lax.broadcasted_iota(jnp.int32, (batch, width), 0)
    lane = lax.broadcasted_iota(jnp.int32, (batch, width), 1)
    half = width // 2
    length = jnp.zeros((batch, width), jnp.int32)
    for b in range(batch):
        length = jnp.where(row == b, lengths[b], length)
    low = lane < half
    exponents = jnp.where(low, lane, lane - half).astype(f32) * (2.0 / width)
    angles = length.astype(f32) * jnp.exp(-exponents * math.log(ROPE_BASE))
    cosine = jnp.cos(angles)
    sine = jnp.where(low, -jnp.sin(angles), jnp.sin(angles))
    usable = (y * RING + x) * span + lane < length
    scale = 1.0 / math.sqrt(width)
    wide_row = lax.broadcasted_iota(jnp.int32, (2 * batch, batch * width), 0)
    wide_col = lax.broadcasted_iota(jnp.int32, (2 * batch, batch * width), 1)
    own_block = jnp.where(lax.rem(wide_row, batch) == wide_col // width, 1.0, 0.0).astype(bf16)
    for part in range(heads // 2):
        diag[pl.ds(part * 2 * batch, 2 * batch), :] = own_block

    def rotate(u):
        return u * cosine + pltpu.roll(u, half, axis=1) * sine

    def spread(tall):
        return jnp.concatenate([tall] * batch, axis=1) * diag[...]

    def ring_copy(out, buf, l, axis, me, phase, d):
        return pltpu.make_async_remote_copy(
            src_ref=out.at[l], dst_ref=buf.at[l, me],
            send_sem=a_send.at[l, phase, d], recv_sem=a_recv.at[l, phase, d],
            device_id={axis: lax.rem(me + d, RING), "tp": swapped}, device_id_type=MESH,
        )

    def ring_start(*args):
        for d in FAR_FIRST:
            ring_copy(*args, d).start()

    def ring_arrive(out, buf, l, axis, me, phase):
        for d in reversed(FAR_FIRST):
            pltpu.make_async_remote_copy(
                src_ref=out.at[l], dst_ref=buf.at[l, lax.rem(me + RING - d, RING)],
                send_sem=a_send.at[l, phase, d], recv_sem=a_recv.at[l, phase, d],
                device_id={axis: lax.rem(me + d, RING), "tp": swapped}, device_id_type=MESH,
            ).wait_recv()

    def ring_sent(*args):
        for d in FAR_FIRST:
            ring_copy(*args, d).wait_send()

    def tp_copy(l, k):
        return pltpu.make_async_remote_copy(
            src_ref=cbuf.at[l, tp], dst_ref=cbuf.at[l, tp],
            send_sem=c_send.at[l, k], recv_sem=c_recv.at[l, k],
            device_id={"tp": tp_partner(TP_STEPS[k])}, device_id_type=MESH,
        )

    def total(buf, l):
        return (buf[l, 0] + buf[l, 1]) + (buf[l, 2] + buf[l, 3])

    def tile(values, i):
        return values[:, i * width:(i + 1) * width]

    def over_lane(values, i):
        return jnp.broadcast_to(values[:, i:i + 1], (batch, width))

    def merge(buf, l):
        group = heads // 2
        stats = [buf[l, s, :, pl.ds(group * width, width)] for s in range(RING)]
        top = functools.reduce(jnp.maximum, stats)
        shrink = [jnp.exp(t - top) for t in stats]
        sums = functools.reduce(
            jnp.add, [pltpu.roll(e, half, axis=1) * t for e, t in zip(shrink, stats)]
        )
        out = []
        for i in range(group):
            parts = [
                over_lane(shrink[s], i) * buf[l, s, :, pl.ds(i * width, width)] for s in range(RING)
            ]
            out.append((parts[0] + parts[1]) + (parts[2] + parts[3]))
        return out, jnp.where(low, top, sums)

    def finish(buf, l, own, new_value):
        group = heads // 2
        stats = [buf[l, s, :, pl.ds(group * width, width)] for s in range(RING)] + [own]
        top = functools.reduce(jnp.maximum, stats)
        shrink = [jnp.exp(t - top) for t in stats]
        sums = functools.reduce(
            jnp.add, [e * pltpu.roll(t, half, axis=1) for e, t in zip(shrink, stats)]
        )
        share = [e / sums for e in shrink]
        out = []
        for i in range(group):
            parts = [
                over_lane(share[s], i) * buf[l, s, :, pl.ds(i * width, width)] for s in range(RING)
            ] + [over_lane(share[RING], i) * new_value]
            out.append((parts[0] + parts[1]) + (parts[2] + parts[3]) + parts[4])
        return out

    hidden_copy.wait()
    gains_copy.wait()

    def layer(l, stream):
        for copy in weight_copies(l):
            copy.wait()
        if l == 0:
            late_start(0)
            for later in range(1, layers):
                for copy in weight_copies(later):
                    copy.start()
                late_start(later)
        gain = gains_v[pl.ds(l, 1), :].astype(f32)
        scaled = (stream * gain).astype(bf16)
        a1xo[l] = jnp.dot(scaled, wqkv[l, :, pl.ds(0, FIRST)], preferred_element_type=f32)
        if l == 0:
            pl.semaphore_wait(barrier, 2 * (RING - 1) + len(TP_STEPS))
        ring_start(a1xo, a1x, l, "ctx_1", x, 0)
        rest = columns + 2 * width - FIRST
        a1yo[l, :, pl.ds(0, rest)] = jnp.dot(
            scaled, wqkv[l, :, pl.ds(FIRST, rest)], preferred_element_type=f32
        )
        squares = stream * stream
        a1yo[l, :, pl.ds(rest, width)] = functools.reduce(
            jnp.add, [tile(squares, i) for i in range(features // width)]
        )
        ring_start(a1yo, a1y, l, "ctx_0", y, 1)

        ring_arrive(a1xo, a1x, l, "ctx_1", x, 0)
        a2yo[l] = total(a1x, l)
        ring_start(a2yo, a2y, l, "ctx_0", y, 2)
        ring_arrive(a1yo, a1y, l, "ctx_0", y, 1)
        a2xo[l] = total(a1y, l)
        ring_start(a2xo, a2x, l, "ctx_1", x, 3)
        ring_arrive(a2yo, a2y, l, "ctx_0", y, 2)
        ring_arrive(a2xo, a2x, l, "ctx_1", x, 3)

        raw = jnp.concatenate([total(a2y, l), total(a2x, l)], axis=1)
        mean = jnp.sum(tile(raw, heads + 2), axis=1, keepdims=True) / (RING * RING * features)
        inverse = lax.rsqrt(mean + NORM_EPS)
        query = [rotate(tile(raw, h) * inverse).astype(bf16) for h in range(heads)]
        tall = jnp.concatenate(query, axis=0)
        pltpu.make_async_copy(kcat.at[l], kcat.at[l], w_sem.at[l, 3]).wait()
        scores = lax.dot_general(
            spread(tall), kcat[l], (((1,), (1,)), ((), ())), preferred_element_type=f32
        ) * scale
        zero = jnp.zeros((batch, width), f32)
        stats_first, stats_last = zero, zero
        weights = []
        for h in range(heads):
            masked = jnp.where(usable, scores[h * batch:(h + 1) * batch], MASK_FILL)
            top = jnp.max(masked, axis=1, keepdims=True)
            weight = jnp.where(usable, jnp.exp(masked - top), 0.0)
            amount = jnp.sum(weight, axis=1, keepdims=True)
            weights.append(weight.astype(bf16))
            i = h % (heads // 2)
            if h < heads // 2:
                stats_first = jnp.where(lane == i, top, jnp.where(lane == half + i, amount, stats_first))
            else:
                stats_last = jnp.where(lane == i, top, jnp.where(lane == half + i, amount, stats_last))
        pltpu.make_async_copy(vc_hbm.at[l], vcat.at[l], w_sem.at[l, 4]).wait()
        sums = jnp.dot(
            spread(jnp.concatenate(weights, axis=0)), vcat[l], preferred_element_type=f32
        )
        group = heads // 2
        for i in range(group):
            b1xo[l, :, pl.ds(i * width, width)] = sums[i * batch:(i + 1) * batch]
        b1xo[l, :, pl.ds(group * width, width)] = stats_first
        ring_start(b1xo, b1x, l, "ctx_1", x, 4)
        for i in range(group):
            b1yo[l, :, pl.ds(i * width, width)] = sums[(group + i) * batch:(group + i + 1) * batch]
        b1yo[l, :, pl.ds(group * width, width)] = stats_last
        ring_start(b1yo, b1y, l, "ctx_0", y, 5)

        new_key = rotate(tile(raw, heads) * inverse).astype(bf16).astype(f32)
        new_value = (tile(raw, heads + 1) * inverse).astype(bf16).astype(f32)
        own = []
        for g in range(2):
            packed = jnp.where(lane >= half, 1.0, 0.0)
            for i in range(group):
                match = jnp.sum(query[g * group + i].astype(f32) * new_key, axis=1, keepdims=True)
                packed = jnp.where(lane == i, match * scale, packed)
            own.append(packed)
        ring_sent(a1xo, a1x, l, "ctx_1", x, 0)
        ring_sent(a1yo, a1y, l, "ctx_0", y, 1)
        ring_sent(a2yo, a2y, l, "ctx_0", y, 2)
        ring_sent(a2xo, a2x, l, "ctx_1", x, 3)

        ring_arrive(b1xo, b1x, l, "ctx_1", x, 4)
        merged, stats = merge(b1x, l)
        for i in range(group):
            b2yo[l, :, pl.ds(i * width, width)] = merged[i]
        b2yo[l, :, pl.ds(group * width, width)] = stats
        ring_start(b2yo, b2y, l, "ctx_0", y, 6)
        ring_arrive(b1yo, b1y, l, "ctx_0", y, 5)
        merged, stats = merge(b1y, l)
        for i in range(group):
            b2xo[l, :, pl.ds(i * width, width)] = merged[i]
        b2xo[l, :, pl.ds(group * width, width)] = stats
        ring_start(b2xo, b2x, l, "ctx_1", x, 7)
        pltpu.make_async_copy(wo_hbm.at[l], wo.at[l], w_sem.at[l, 5]).wait()
        ring_arrive(b2yo, b2y, l, "ctx_0", y, 6)
        context = finish(b2y, l, own[0], new_value)
        ring_arrive(b2xo, b2x, l, "ctx_1", x, 7)
        context = context + finish(b2x, l, own[1], new_value)
        context = jnp.concatenate(context, axis=1).astype(bf16)
        cbuf[l, tp] = jnp.dot(context, wo[l], preferred_element_type=f32)
        for k in range(len(TP_STEPS)):
            tp_copy(l, k).start()
        ring_sent(b1xo, b1x, l, "ctx_1", x, 4)
        ring_sent(b1yo, b1y, l, "ctx_0", y, 5)
        ring_sent(b2yo, b2y, l, "ctx_0", y, 6)
        ring_sent(b2xo, b2x, l, "ctx_1", x, 7)
        for k in reversed(range(len(TP_STEPS))):
            tp_copy(l, k).wait_recv()
        parts = [cbuf[l, t] for t in range(2 * RING)]
        stream = stream + (
            ((parts[0] + parts[1]) + (parts[2] + parts[3])) + ((parts[4] + parts[5]) + (parts[6] + parts[7]))
        )
        for k in range(len(TP_STEPS)):
            tp_copy(l, k).wait_send()
        return stream

    stream = hidden_v[...].astype(f32)
    for l in range(layers):
        stream = layer(l, stream)
    out_ref[...] = stream


def on_device(hidden, norm_gains, w_query, w_key, w_value, w_out, key_cache, value_cache, lengths):
    layers, features, columns = w_query.shape
    batch, _, span, width = key_cache.shape[1:]
    heads = columns // width
    keys = key_cache.reshape(layers, batch, span, width)
    values = value_cache.reshape(layers, batch * span, width)
    f32, bf16 = jnp.float32, jnp.bfloat16
    total = columns + 2 * width
    last = total - FIRST + width
    packed = (heads // 2 + 1) * width
    messages = (FIRST, last, FIRST, last, packed, packed, packed, packed)
    return pl.pallas_call(
        functools.partial(kernel, layers, batch, heads, width, span, features),
        out_shape=jax.ShapeDtypeStruct((batch, features), f32),
        in_specs=[pl.BlockSpec(memory_space=pltpu.HBM)] * 9,
        out_specs=pl.BlockSpec(memory_space=pltpu.VMEM),
        scratch_shapes=[
            pltpu.SMEM((batch,), jnp.int32),
            pltpu.VMEM((batch, features), bf16),
            pltpu.VMEM((layers, features), bf16),
            pltpu.VMEM((layers, features, total), bf16),
            pltpu.VMEM((layers, columns, features), bf16),
            pltpu.VMEM((layers, span, batch * width), bf16),
            pltpu.VMEM((layers, batch * span, width), bf16),
            pltpu.VMEM((heads * batch, batch * width), bf16),
            *[pltpu.VMEM((layers, RING, batch, w), f32) for w in messages],
            *[pltpu.VMEM((layers, batch, w), f32) for w in messages],
            pltpu.VMEM((layers, 2 * RING, batch, features), f32),
            pltpu.SemaphoreType.DMA((3,)),
            pltpu.SemaphoreType.DMA((layers, 6)),
            pltpu.SemaphoreType.DMA((layers, 8, RING)),
            pltpu.SemaphoreType.DMA((layers, 8, RING)),
            pltpu.SemaphoreType.DMA((layers, len(TP_STEPS))),
            pltpu.SemaphoreType.DMA((layers, len(TP_STEPS))),
        ],
        compiler_params=pltpu.CompilerParams(
            collective_id=0, has_side_effects=True, vmem_limit_bytes=48 * 1024 * 1024
        ),
    )(*[pltpu.with_memory_space_constraint(a, pltpu.HBM) for a in (hidden, norm_gains, w_query, w_key, w_value, w_out, keys, values, lengths)])


def solution(mesh):
    finer = Mesh(mesh.devices.reshape(RING, RING, mesh.shape["tp"]), CTX + ("tp",))
    return jax.shard_map(
        on_device,
        mesh=finer,
        in_specs=(
            P(None, CTX),
            P(None, CTX),
            P(None, CTX, "tp"),
            P(None, CTX, "tp"),
            P(None, CTX, "tp"),
            P(None, "tp", CTX),
            P(None, None, "tp", CTX, None),
            P(None, None, "tp", CTX, None),
            P(),
        ),
        out_specs=P(None, CTX),
        check_vma=False,
    )
```

```python
import functools
import math

import jax
import jax.numpy as jnp
from jax import lax
from jax.experimental import pallas as pl
from jax.experimental.pallas import tpu as pltpu
from jax.sharding import Mesh
from jax.sharding import PartitionSpec as P

CTX = ("ctx_0", "ctx_1")
MESH = pl.DeviceIdType.MESH
NORM_EPS = 1e-05
ROPE_BASE = 500000.0
MASK_FILL = -1e30
RING = 4
FAR_FIRST = (2, 1, 3, 0)
TP_STEPS = ((2, 0), (2, 1), (1, 0), (1, 1), (3, 0), (3, 1), (0, 1))
A_PARTS = ((True, (0, 1), 1), (False, (4, 5), 0), (True, (2, 3), 0), (False, (6, 7), 0), (False, (8, 9), 0))
B_PARTS = ((True, (0, 1), 1), (False, (4, 5), 1), (True, (2, 3), 0), (False, (6, 7), 0))
PARTS = A_PARTS + B_PARTS
C_PARTS = 2


def kernel(
    layers, batch, heads, width, span, features,
    hidden_hbm, gains_hbm, wq_hbm, wk_hbm, wv_hbm, wo_hbm, kc_hbm, vc_hbm, lengths_hbm,
    out_ref,
    lengths, hidden_v, gains_v, wqkv, wo, kcat, vcat, diag,
    *rest,
):
    y = lax.axis_index("ctx_0")
    x = lax.axis_index("ctx_1")
    tp = lax.axis_index("tp")
    z, core = tp // 2, lax.rem(tp, 2)
    n = len(PARTS)
    arrived, sent, (cbuf, in_sem, w_sem, p_send, p_recv, c_send, c_recv) = rest[:2 * n], rest[2 * n:4 * n], rest[4 * n:]
    columns = heads * width
    f32, bf16 = jnp.float32, jnp.bfloat16

    def tp_partner(step, sign=1):
        dz, other = step
        zz = lax.rem(z + (dz if sign > 0 else RING - dz), RING)
        cc = 1 - core if other else core
        return zz * 2 + cc

    barrier = pltpu.get_barrier_semaphore()
    swapped = tp + 1 - 2 * core
    for d in FAR_FIRST[:-1]:
        pl.semaphore_signal(
            barrier, inc=1, device_id={"ctx_1": lax.rem(x + d, RING), "tp": swapped}, device_id_type=MESH
        )
        pl.semaphore_signal(
            barrier, inc=1, device_id={"ctx_0": lax.rem(y + d, RING), "tp": swapped}, device_id_type=MESH
        )
    for step in TP_STEPS:
        pl.semaphore_signal(barrier, inc=1, device_id={"tp": tp_partner(step)}, device_id_type=MESH)

    def weight_copies(l):
        return (
            pltpu.make_async_copy(wq_hbm.at[l], wqkv.at[l, :, pl.ds(0, columns)], w_sem.at[l, 0]),
            pltpu.make_async_copy(wk_hbm.at[l], wqkv.at[l, :, pl.ds(columns, width)], w_sem.at[l, 1]),
            pltpu.make_async_copy(wv_hbm.at[l], wqkv.at[l, :, pl.ds(columns + width, width)], w_sem.at[l, 2]),
        )

    def late_start(l):
        for b in range(batch):
            pltpu.make_async_copy(
                kc_hbm.at[l, b], kcat.at[l, :, pl.ds(b * width, width)], w_sem.at[l, 3]
            ).start()
        pltpu.make_async_copy(vc_hbm.at[l], vcat.at[l], w_sem.at[l, 4]).start()
        pltpu.make_async_copy(wo_hbm.at[l], wo.at[l], w_sem.at[l, 5]).start()

    hidden_copy = pltpu.make_async_copy(hidden_hbm, hidden_v, in_sem.at[0])
    gains_copy = pltpu.make_async_copy(gains_hbm, gains_v, in_sem.at[1])
    lengths_copy = pltpu.make_async_copy(lengths_hbm, lengths, in_sem.at[2])
    lengths_copy.start()
    hidden_copy.start()
    gains_copy.start()
    for copy in weight_copies(0):
        copy.start()

    lengths_copy.wait()
    row = lax.broadcasted_iota(jnp.int32, (batch, width), 0)
    lane = lax.broadcasted_iota(jnp.int32, (batch, width), 1)
    half = width // 2
    length = jnp.zeros((batch, width), jnp.int32)
    for b in range(batch):
        length = jnp.where(row == b, lengths[b], length)
    low = lane < half
    exponents = jnp.where(low, lane, lane - half).astype(f32) * (2.0 / width)
    angles = length.astype(f32) * jnp.exp(-exponents * math.log(ROPE_BASE))
    cosine = jnp.cos(angles)
    sine = jnp.where(low, -jnp.sin(angles), jnp.sin(angles))
    usable = (y * RING + x) * span + lane < length
    scale = 1.0 / math.sqrt(width)
    wide_row = lax.broadcasted_iota(jnp.int32, (2 * batch, batch * width), 0)
    wide_col = lax.broadcasted_iota(jnp.int32, (2 * batch, batch * width), 1)
    own_block = jnp.where(lax.rem(wide_row, batch) == wide_col // width, 1.0, 0.0).astype(bf16)
    for part in range(heads // 2):
        diag[pl.ds(part * 2 * batch, 2 * batch), :] = own_block

    def spread(tall):
        return jnp.concatenate([tall] * batch, axis=1) * diag[...]

    def start(l, p, e):
        axis, me = ("ctx_1", x) if PARTS[p][0] == (e == 0) else ("ctx_0", y)
        for d in FAR_FIRST:
            pltpu.make_async_remote_copy(
                src_ref=sent[2 * p + e].at[l], dst_ref=arrived[2 * p + e].at[l, me],
                send_sem=p_send.at[l, p, e], recv_sem=p_recv.at[l, p, e],
                device_id={axis: lax.rem(me + d, RING), "tp": swapped}, device_id_type=MESH,
            ).start()

    def bytes_of(ref, sem):
        pltpu.make_async_copy(ref, ref, sem).wait()

    def arrive(l, p, e):
        bytes_of(arrived[2 * p + e].at[l], p_recv.at[l, p, e])

    def all_sent(l, parts):
        for p in parts:
            for e in range(2):
                bytes_of(arrived[2 * p + e].at[l], p_send.at[l, p, e])

    def tp_start(l, part):
        for step in TP_STEPS:
            pltpu.make_async_remote_copy(
                src_ref=cbuf.at[l, part, tp], dst_ref=cbuf.at[l, part, tp],
                send_sem=c_send.at[l, part], recv_sem=c_recv.at[l, part],
                device_id={"tp": tp_partner(step)}, device_id_type=MESH,
            ).start()

    def total(l, p, e):
        buf = arrived[2 * p + e]
        return (buf[l, 0] + buf[l, 1]) + (buf[l, 2] + buf[l, 3])

    def tile(values, i):
        return values[:, i * width:(i + 1) * width]

    def over_lane(values, i):
        return jnp.broadcast_to(values[:, i:i + 1], (batch, width))

    def weighted(l, p, e, factors):
        buf = arrived[2 * p + e]
        out = []
        for k, h in enumerate(PARTS[p][1]):
            terms = [
                over_lane(factors[s], h % (heads // 2)) * buf[l, s, :, pl.ds(k * width, width)]
                for s in range(RING)
            ]
            out.append((terms[0] + terms[1]) + (terms[2] + terms[3]))
        return out

    def stats_of(l, p, e):
        at = len(PARTS[p][1]) * width
        return [arrived[2 * p + e][l, s, :, pl.ds(at, width)] for s in range(RING)]

    def put(l, p, e, tiles):
        for k, t in enumerate(tiles):
            sent[2 * p + e][l, :, pl.ds(k * width, width)] = t

    hidden_copy.wait()
    gains_copy.wait()

    def layer(l, stream):
        for copy in weight_copies(l):
            copy.wait()
        if l == 0:
            late_start(0)
            for later in range(1, layers):
                for copy in weight_copies(later):
                    copy.start()
                late_start(later)
        gain = gains_v[pl.ds(l, 1), :].astype(f32)
        scaled = (stream * gain).astype(bf16)
        squares = stream * stream
        squares = functools.reduce(jnp.add, [tile(squares, i) for i in range(features // width)])
        products = [
            jnp.dot(scaled, wqkv[l, :, pl.ds(hs[0] * width, len(hs) * width)], preferred_element_type=f32)
            for _, hs, _ in A_PARTS
        ]
        a_ids, b_ids = range(len(A_PARTS)), range(len(A_PARTS), n)
        for p in a_ids:
            sent[2 * p][l, :, pl.ds(0, 2 * width)] = products[p]
            if PARTS[p][2]:
                sent[2 * p][l, :, pl.ds(2 * width, width)] = squares
            if l == 0 and p == 0:
                pl.semaphore_wait(barrier, 2 * (RING - 1) + len(TP_STEPS))
            start(l, p, 0)
        for p in a_ids:
            arrive(l, p, 0)
            sent[2 * p + 1][l] = total(l, p, 0)
            start(l, p, 1)

        query = [None] * heads
        for p in a_ids[:-1]:
            arrive(l, p, 1)
            raw = total(l, p, 1)
            if PARTS[p][2]:
                mean = jnp.sum(tile(raw, 2), axis=1, keepdims=True) / (RING * RING * features)
                inverse = jnp.broadcast_to(lax.rsqrt(mean + NORM_EPS), (batch, width))
                turn_cos, turn_sin = cosine * inverse, sine * inverse
            for k, h in enumerate(PARTS[p][1]):
                u = tile(raw, k)
                query[h] = (u * turn_cos + pltpu.roll(u, half, axis=1) * turn_sin).astype(bf16)
        tall = jnp.concatenate(query, axis=0)
        bytes_of(kcat.at[l], w_sem.at[l, 3])
        scores = lax.dot_general(
            spread(tall), kcat[l], (((1,), (1,)), ((), ())), preferred_element_type=f32
        ) * scale
        group = heads // 2
        stats = [jnp.zeros((batch, width), f32)] * 2
        weights = []
        for h in range(heads):
            masked = jnp.where(usable, scores[h * batch:(h + 1) * batch], MASK_FILL)
            top = jnp.max(masked, axis=1, keepdims=True)
            weight = jnp.where(usable, jnp.exp(masked - top), 0.0)
            amount = jnp.sum(weight, axis=1, keepdims=True)
            weights.append(weight.astype(bf16))
            i = h % group
            stats[h // group] = jnp.where(
                lane == i, top, jnp.where(lane == half + i, amount, stats[h // group])
            )
        bytes_of(vcat.at[l], w_sem.at[l, 4])
        sums = jnp.dot(
            spread(jnp.concatenate(weights, axis=0)), vcat[l], preferred_element_type=f32
        )
        for p in b_ids:
            _, hs, more = PARTS[p]
            put(l, p, 0, [sums[h * batch:(h + 1) * batch] for h in hs] + [stats[hs[0] // group]] * more)
            start(l, p, 0)

        p = a_ids[-1]
        arrive(l, p, 1)
        raw = total(l, p, 1)
        u = tile(raw, 0)
        new_key = (u * turn_cos + pltpu.roll(u, half, axis=1) * turn_sin).astype(bf16).astype(f32)
        new_value = (tile(raw, 1) * inverse).astype(bf16).astype(f32)
        own = []
        for g in range(2):
            packed = jnp.where(lane >= half, 1.0, 0.0)
            for i in range(group):
                match = jnp.sum(query[g * group + i].astype(f32) * new_key, axis=1, keepdims=True)
                packed = jnp.where(lane == i, match * scale, packed)
            own.append(packed)
        all_sent(l, a_ids)
        bytes_of(wo.at[l], w_sem.at[l, 5])

        shrink = [None, None]
        for p in b_ids:
            arrive(l, p, 0)
            _, hs, more = PARTS[p]
            g = hs[0] // group
            tiles = []
            if more:
                each = stats_of(l, p, 0)
                top = functools.reduce(jnp.maximum, each)
                shrink[g] = [jnp.exp(t - top) for t in each]
                amount = functools.reduce(
                    jnp.add, [pltpu.roll(e, half, axis=1) * t for e, t in zip(shrink[g], each)]
                )
                tiles = [jnp.where(low, top, amount)]
            put(l, p, 1, weighted(l, p, 0, shrink[g]) + tiles)
            start(l, p, 1)

        share = [None, None]
        out = [None] * C_PARTS
        piece = features // C_PARTS
        for p in b_ids:
            arrive(l, p, 1)
            _, hs, more = PARTS[p]
            g = hs[0] // group
            if more:
                each = stats_of(l, p, 1) + [own[g]]
                top = functools.reduce(jnp.maximum, each)
                factors = [jnp.exp(t - top) for t in each]
                amount = functools.reduce(
                    jnp.add, [e * pltpu.roll(t, half, axis=1) for e, t in zip(factors, each)]
                )
                share[g] = [e / amount for e in factors]
            context = [
                v + over_lane(share[g][RING], h % group) * new_value
                for v, h in zip(weighted(l, p, 1, share[g]), hs)
            ]
            context = jnp.concatenate(context, axis=1).astype(bf16)
            for c in range(C_PARTS):
                product = jnp.dot(
                    context, wo[l, pl.ds(hs[0] * width, len(hs) * width), pl.ds(c * piece, piece)],
                    preferred_element_type=f32,
                )
                out[c] = product if out[c] is None else out[c] + product
        for c in range(C_PARTS):
            cbuf[l, c, tp] = out[c]
            tp_start(l, c)
        all_sent(l, b_ids)
        pieces = []
        for c in range(C_PARTS):
            bytes_of(cbuf.at[l, c, pl.ds(0, len(TP_STEPS))], c_recv.at[l, c])
            t = [cbuf[l, c, i] for i in range(2 * RING)]
            pieces.append(((t[0] + t[1]) + (t[2] + t[3])) + ((t[4] + t[5]) + (t[6] + t[7])))
        stream = stream + jnp.concatenate(pieces, axis=1)
        for c in range(C_PARTS):
            bytes_of(cbuf.at[l, c, pl.ds(0, len(TP_STEPS))], c_send.at[l, c])
        return stream

    stream = hidden_v[...].astype(f32)
    for l in range(layers):
        stream = layer(l, stream)
    out_ref[...] = stream


def on_device(hidden, norm_gains, w_query, w_key, w_value, w_out, key_cache, value_cache, lengths):
    layers, features, columns = w_query.shape
    batch, _, span, width = key_cache.shape[1:]
    heads = columns // width
    keys = key_cache.reshape(layers, batch, span, width)
    values = value_cache.reshape(layers, batch * span, width)
    f32, bf16 = jnp.float32, jnp.bfloat16
    messages = [(len(hs) + more) * width for _, hs, more in PARTS for _ in range(2)]
    return pl.pallas_call(
        functools.partial(kernel, layers, batch, heads, width, span, features),
        out_shape=jax.ShapeDtypeStruct((batch, features), f32),
        in_specs=[pl.BlockSpec(memory_space=pltpu.HBM)] * 9,
        out_specs=pl.BlockSpec(memory_space=pltpu.VMEM),
        scratch_shapes=[
            pltpu.SMEM((batch,), jnp.int32),
            pltpu.VMEM((batch, features), bf16),
            pltpu.VMEM((layers, features), bf16),
            pltpu.VMEM((layers, features, columns + 2 * width), bf16),
            pltpu.VMEM((layers, columns, features), bf16),
            pltpu.VMEM((layers, span, batch * width), bf16),
            pltpu.VMEM((layers, batch * span, width), bf16),
            pltpu.VMEM((heads * batch, batch * width), bf16),
            *[pltpu.VMEM((layers, RING, batch, w), f32) for w in messages],
            *[pltpu.VMEM((layers, batch, w), f32) for w in messages],
            pltpu.VMEM((layers, C_PARTS, 2 * RING, batch, features // C_PARTS), f32),
            pltpu.SemaphoreType.DMA((3,)),
            pltpu.SemaphoreType.DMA((layers, 6)),
            pltpu.SemaphoreType.DMA((layers, len(PARTS), 2)),
            pltpu.SemaphoreType.DMA((layers, len(PARTS), 2)),
            pltpu.SemaphoreType.DMA((layers, C_PARTS)),
            pltpu.SemaphoreType.DMA((layers, C_PARTS)),
        ],
        compiler_params=pltpu.CompilerParams(
            collective_id=0, has_side_effects=True, vmem_limit_bytes=48 * 1024 * 1024
        ),
    )(*[pltpu.with_memory_space_constraint(a, pltpu.HBM) for a in (hidden, norm_gains, w_query, w_key, w_value, w_out, keys, values, lengths)])


def solution(mesh):
    finer = Mesh(mesh.devices.reshape(RING, RING, mesh.shape["tp"]), CTX + ("tp",))
    return jax.shard_map(
        on_device,
        mesh=finer,
        in_specs=(
            P(None, CTX),
            P(None, CTX),
            P(None, CTX, "tp"),
            P(None, CTX, "tp"),
            P(None, CTX, "tp"),
            P(None, "tp", CTX),
            P(None, None, "tp", CTX, None),
            P(None, None, "tp", CTX, None),
            P(),
        ),
        out_specs=P(None, CTX),
        check_vma=False,
    )
```

```python
import functools
import math

import jax
import jax.numpy as jnp
from jax import lax
from jax.experimental import pallas as pl
from jax.experimental.pallas import tpu as pltpu
from jax.sharding import Mesh
from jax.sharding import PartitionSpec as P

CTX = ("ctx_0", "ctx_1")
MESH = pl.DeviceIdType.MESH
NORM_EPS = 1e-05
ROPE_BASE = 500000.0
MASK_FILL = -1e30
RING = 4
FAR_FIRST = (2, 1, 3, 0)
TP_STEPS = ((2, 0), (2, 1), (1, 0), (1, 1), (3, 0), (3, 1), (0, 1))
A_PARTS = ((True, (0, 1), 1), (False, (2, 3, 4), 0), (True, (5, 6, 7), 0), (False, (8, 9), 0))
B_PARTS = ((True, (0, 1), 1), (False, (4, 5), 1), (True, (2, 3), 0), (False, (6, 7), 0))
PARTS = A_PARTS + B_PARTS
C_PARTS = 1


def kernel(
    layers, batch, heads, width, span, features,
    hidden_hbm, gains_hbm, wq_hbm, wk_hbm, wv_hbm, wo_hbm, kc_hbm, vc_hbm, lengths_hbm,
    out_ref,
    lengths, hidden_v, gains_v, wqkv, wo, kcat, vcat, turned, diag,
    *rest,
):
    y = lax.axis_index("ctx_0")
    x = lax.axis_index("ctx_1")
    tp = lax.axis_index("tp")
    z, core = tp // 2, lax.rem(tp, 2)
    n = len(PARTS)
    arrived, sent, (cbuf, in_sem, w_sem, wq_sem, p_send, p_recv, c_send, c_recv) = rest[:2 * n], rest[2 * n:4 * n], rest[4 * n:]
    columns = heads * width
    f32, bf16 = jnp.float32, jnp.bfloat16

    def tp_partner(step, sign=1):
        dz, other = step
        zz = lax.rem(z + (dz if sign > 0 else RING - dz), RING)
        cc = 1 - core if other else core
        return zz * 2 + cc

    barrier = pltpu.get_barrier_semaphore()
    swapped = tp + 1 - 2 * core
    for d in FAR_FIRST[:-1]:
        pl.semaphore_signal(
            barrier, inc=1, device_id={"ctx_1": lax.rem(x + d, RING), "tp": swapped}, device_id_type=MESH
        )
        pl.semaphore_signal(
            barrier, inc=1, device_id={"ctx_0": lax.rem(y + d, RING), "tp": swapped}, device_id_type=MESH
        )
    for step in TP_STEPS:
        pl.semaphore_signal(barrier, inc=1, device_id={"tp": tp_partner(step)}, device_id_type=MESH)

    def weight_copies(l):
        copies = []
        for p, (_, hs, _) in enumerate(A_PARTS[:-1]):
            at = pl.ds(hs[0] * width, len(hs) * width)
            copies.append(pltpu.make_async_copy(wq_hbm.at[l, :, at], wqkv.at[l, :, at], wq_sem.at[l, p]))
        return copies + [
            pltpu.make_async_copy(wk_hbm.at[l], wqkv.at[l, :, pl.ds(columns, width)], w_sem.at[l, 1]),
            pltpu.make_async_copy(wv_hbm.at[l], wqkv.at[l, :, pl.ds(columns + width, width)], w_sem.at[l, 2]),
        ]

    def late_start(l):
        for b in range(batch):
            pltpu.make_async_copy(
                kc_hbm.at[l, b], kcat.at[l, :, pl.ds(b * width, width)], w_sem.at[l, 3]
            ).start()
        pltpu.make_async_copy(vc_hbm.at[l], vcat.at[l], w_sem.at[l, 4]).start()
        pltpu.make_async_copy(wo_hbm.at[l], wo.at[l], w_sem.at[l, 5]).start()

    hidden_copy = pltpu.make_async_copy(hidden_hbm, hidden_v, in_sem.at[0])
    gains_copy = pltpu.make_async_copy(gains_hbm, gains_v, in_sem.at[1])
    lengths_copy = pltpu.make_async_copy(lengths_hbm, lengths, in_sem.at[2])
    hidden_copy.start()
    gains_copy.start()
    for copy in weight_copies(0):
        copy.start()
    lengths_copy.start()

    lengths_copy.wait()
    row = lax.broadcasted_iota(jnp.int32, (batch, width), 0)
    lane = lax.broadcasted_iota(jnp.int32, (batch, width), 1)
    half = width // 2
    length = jnp.zeros((batch, width), jnp.int32)
    for b in range(batch):
        length = jnp.where(row == b, lengths[b], length)
    low = lane < half
    exponents = jnp.where(low, lane, lane - half).astype(f32) * (2.0 / width)
    angles = length.astype(f32) * jnp.exp(-exponents * math.log(ROPE_BASE))
    cosine = jnp.cos(angles)
    sine = jnp.where(low, -jnp.sin(angles), jnp.sin(angles))
    usable = (y * RING + x) * span + lane < length
    scale = 1.0 / math.sqrt(width)
    wide_row = lax.broadcasted_iota(jnp.int32, (2 * batch, batch * width), 0)
    wide_col = lax.broadcasted_iota(jnp.int32, (2 * batch, batch * width), 1)
    own_block = jnp.where(lax.rem(wide_row, batch) == wide_col // width, 1.0, 0.0).astype(bf16)
    for part in range(heads // 2):
        diag[pl.ds(part * 2 * batch, 2 * batch), :] = own_block

    def spread(tall):
        return jnp.concatenate([tall] * batch, axis=1) * diag[...]

    def start(l, p, e):
        axis, me = ("ctx_1", x) if PARTS[p][0] == (e == 0) else ("ctx_0", y)
        for d in FAR_FIRST:
            pltpu.make_async_remote_copy(
                src_ref=sent[2 * p + e].at[l], dst_ref=arrived[2 * p + e].at[l, me],
                send_sem=p_send.at[l, p, e], recv_sem=p_recv.at[l, p, e],
                device_id={axis: lax.rem(me + d, RING), "tp": swapped}, device_id_type=MESH,
            ).start()

    def bytes_of(ref, sem):
        pltpu.make_async_copy(ref, ref, sem).wait()

    def arrive(l, p, e):
        bytes_of(arrived[2 * p + e].at[l], p_recv.at[l, p, e])

    def all_sent(l, parts):
        for p in parts:
            for e in range(2):
                bytes_of(arrived[2 * p + e].at[l], p_send.at[l, p, e])

    def tp_start(l, part):
        for step in TP_STEPS:
            pltpu.make_async_remote_copy(
                src_ref=cbuf.at[l, part, tp], dst_ref=cbuf.at[l, part, tp],
                send_sem=c_send.at[l, part], recv_sem=c_recv.at[l, part],
                device_id={"tp": tp_partner(step)}, device_id_type=MESH,
            ).start()

    def total(l, p, e):
        buf = arrived[2 * p + e]
        return (buf[l, 0] + buf[l, 1]) + (buf[l, 2] + buf[l, 3])

    def tile(values, i):
        return values[:, i * width:(i + 1) * width]

    def over_lane(values, i):
        return jnp.broadcast_to(values[:, i:i + 1], (batch, width))

    def weighted(l, p, e, factors):
        buf = arrived[2 * p + e]
        out = []
        for k, h in enumerate(PARTS[p][1]):
            terms = [
                over_lane(factors[s], h % (heads // 2)) * buf[l, s, :, pl.ds(k * width, width)]
                for s in range(RING)
            ]
            out.append((terms[0] + terms[1]) + (terms[2] + terms[3]))
        return out

    def stats_of(l, p, e):
        at = len(PARTS[p][1]) * width
        return [arrived[2 * p + e][l, s, :, pl.ds(at, width)] for s in range(RING)]

    def put(l, p, e, tiles):
        for k, t in enumerate(tiles):
            sent[2 * p + e][l, :, pl.ds(k * width, width)] = t

    hidden_copy.wait()
    gains_copy.wait()

    def layer(l, stream):
        copies = weight_copies(l)
        if l > 0:
            for copy in copies:
                copy.wait()
        gain = gains_v[pl.ds(l, 1), :].astype(f32)
        scaled = (stream * gain).astype(bf16)
        squares = stream * stream
        squares = functools.reduce(jnp.add, [tile(squares, i) for i in range(features // width)])
        products = []
        for p, (_, hs, _) in enumerate(A_PARTS):
            if l == 0:
                for copy in copies[p:p + 1] if p < len(A_PARTS) - 1 else copies[p:]:
                    copy.wait()
            products.append(
                jnp.dot(scaled, wqkv[l, :, pl.ds(hs[0] * width, len(hs) * width)], preferred_element_type=f32)
            )
        a_ids, b_ids = range(len(A_PARTS)), range(len(A_PARTS), n)
        for p in a_ids:
            sent[2 * p][l, :, pl.ds(0, len(PARTS[p][1]) * width)] = products[p]
            if PARTS[p][2]:
                sent[2 * p][l, :, pl.ds(2 * width, width)] = squares
            if l == 0 and p == 0:
                pl.semaphore_wait(barrier, 2 * (RING - 1) + len(TP_STEPS))
            start(l, p, 0)
        if l == 0:
            late_start(0)
        for p in a_ids:
            arrive(l, p, 0)
            sent[2 * p + 1][l] = total(l, p, 0)
            start(l, p, 1)
        if l + 1 < layers:
            for copy in weight_copies(l + 1):
                copy.start()
        bytes_of(kcat.at[l], w_sem.at[l, 3])
        turned[...] = kcat[l].T

        query = [None] * heads
        for p in a_ids[:-1]:
            arrive(l, p, 1)
            raw = total(l, p, 1)
            if PARTS[p][2]:
                mean = jnp.sum(tile(raw, 2), axis=1, keepdims=True) / (RING * RING * features)
                inverse = jnp.broadcast_to(lax.rsqrt(mean + NORM_EPS), (batch, width))
                turn_cos, turn_sin = cosine * inverse, sine * inverse
            for k, h in enumerate(PARTS[p][1]):
                u = tile(raw, k)
                query[h] = (u * turn_cos + pltpu.roll(u, half, axis=1) * turn_sin).astype(bf16)
        tall = jnp.concatenate(query, axis=0)
        scores = lax.dot_general(
            spread(tall), turned[...], (((1,), (0,)), ((), ())), preferred_element_type=f32
        ) * scale
        group = heads // 2
        stats = [jnp.zeros((batch, width), f32)] * 2
        weights = []
        for h in range(heads):
            masked = jnp.where(usable, scores[h * batch:(h + 1) * batch], MASK_FILL)
            top = jnp.max(masked, axis=1, keepdims=True)
            weight = jnp.where(usable, jnp.exp(masked - top), 0.0)
            amount = jnp.sum(weight, axis=1, keepdims=True)
            weights.append(weight.astype(bf16))
            i = h % group
            stats[h // group] = jnp.where(
                lane == i, top, jnp.where(lane == half + i, amount, stats[h // group])
            )
        bytes_of(vcat.at[l], w_sem.at[l, 4])
        sums = jnp.dot(
            spread(jnp.concatenate(weights, axis=0)), vcat[l], preferred_element_type=f32
        )
        for p in b_ids:
            _, hs, more = PARTS[p]
            put(l, p, 0, [sums[h * batch:(h + 1) * batch] for h in hs] + [stats[hs[0] // group]] * more)
            start(l, p, 0)

        if l + 1 < layers:
            late_start(l + 1)

        p = a_ids[-1]
        arrive(l, p, 1)
        raw = total(l, p, 1)
        u = tile(raw, 0)
        new_key = (u * turn_cos + pltpu.roll(u, half, axis=1) * turn_sin).astype(bf16).astype(f32)
        new_value = (tile(raw, 1) * inverse).astype(bf16).astype(f32)
        own = []
        for g in range(2):
            packed = jnp.where(lane >= half, 1.0, 0.0)
            for i in range(group):
                match = jnp.sum(query[g * group + i].astype(f32) * new_key, axis=1, keepdims=True)
                packed = jnp.where(lane == i, match * scale, packed)
            own.append(packed)
        all_sent(l, a_ids)
        bytes_of(wo.at[l], w_sem.at[l, 5])

        shrink = [None, None]
        for p in b_ids:
            arrive(l, p, 0)
            _, hs, more = PARTS[p]
            g = hs[0] // group
            tiles = []
            if more:
                each = stats_of(l, p, 0)
                top = functools.reduce(jnp.maximum, each)
                shrink[g] = [jnp.exp(t - top) for t in each]
                amount = functools.reduce(
                    jnp.add, [pltpu.roll(e, half, axis=1) * t for e, t in zip(shrink[g], each)]
                )
                tiles = [jnp.where(low, top, amount)]
            put(l, p, 1, weighted(l, p, 0, shrink[g]) + tiles)
            start(l, p, 1)

        share = [None, None]
        out = [None] * C_PARTS
        piece = features // C_PARTS
        for p in b_ids:
            arrive(l, p, 1)
            _, hs, more = PARTS[p]
            g = hs[0] // group
            if more:
                each = stats_of(l, p, 1) + [own[g]]
                top = functools.reduce(jnp.maximum, each)
                factors = [jnp.exp(t - top) for t in each]
                amount = functools.reduce(
                    jnp.add, [e * pltpu.roll(t, half, axis=1) for e, t in zip(factors, each)]
                )
                share[g] = [e / amount for e in factors]
            context = [
                v + over_lane(share[g][RING], h % group) * new_value
                for v, h in zip(weighted(l, p, 1, share[g]), hs)
            ]
            context = jnp.concatenate(context, axis=1).astype(bf16)
            for c in range(C_PARTS):
                product = jnp.dot(
                    context, wo[l, pl.ds(hs[0] * width, len(hs) * width), pl.ds(c * piece, piece)],
                    preferred_element_type=f32,
                )
                out[c] = product if out[c] is None else out[c] + product
        for c in range(C_PARTS):
            cbuf[l, c, tp] = out[c]
            tp_start(l, c)
        all_sent(l, b_ids)
        pieces = []
        for c in range(C_PARTS):
            bytes_of(cbuf.at[l, c, pl.ds(0, len(TP_STEPS))], c_recv.at[l, c])
            t = [cbuf[l, c, i] for i in range(2 * RING)]
            pieces.append(((t[0] + t[1]) + (t[2] + t[3])) + ((t[4] + t[5]) + (t[6] + t[7])))
        stream = stream + jnp.concatenate(pieces, axis=1)
        for c in range(C_PARTS):
            bytes_of(cbuf.at[l, c, pl.ds(0, len(TP_STEPS))], c_send.at[l, c])
        return stream

    stream = hidden_v[...].astype(f32)
    for l in range(layers):
        stream = layer(l, stream)
    out_ref[...] = stream


def on_device(hidden, norm_gains, w_query, w_key, w_value, w_out, key_cache, value_cache, lengths):
    layers, features, columns = w_query.shape
    batch, _, span, width = key_cache.shape[1:]
    heads = columns // width
    keys = key_cache.reshape(layers, batch, span, width)
    values = value_cache.reshape(layers, batch * span, width)
    f32, bf16 = jnp.float32, jnp.bfloat16
    messages = [(len(hs) + more) * width for _, hs, more in PARTS for _ in range(2)]
    return pl.pallas_call(
        functools.partial(kernel, layers, batch, heads, width, span, features),
        out_shape=jax.ShapeDtypeStruct((batch, features), f32),
        in_specs=[pl.BlockSpec(memory_space=pltpu.HBM)] * 9,
        out_specs=pl.BlockSpec(memory_space=pltpu.VMEM),
        scratch_shapes=[
            pltpu.SMEM((batch,), jnp.int32),
            pltpu.VMEM((batch, features), bf16),
            pltpu.VMEM((layers, features), bf16),
            pltpu.VMEM((layers, features, columns + 2 * width), bf16),
            pltpu.VMEM((layers, columns, features), bf16),
            pltpu.VMEM((layers, span, batch * width), bf16),
            pltpu.VMEM((layers, batch * span, width), bf16),
            pltpu.VMEM((batch * width, span), bf16),
            pltpu.VMEM((heads * batch, batch * width), bf16),
            *[pltpu.VMEM((layers, RING, batch, w), f32) for w in messages],
            *[pltpu.VMEM((layers, batch, w), f32) for w in messages],
            pltpu.VMEM((layers, C_PARTS, 2 * RING, batch, features // C_PARTS), f32),
            pltpu.SemaphoreType.DMA((3,)),
            pltpu.SemaphoreType.DMA((layers, 6)),
            pltpu.SemaphoreType.DMA((layers, len(A_PARTS) - 1)),
            pltpu.SemaphoreType.DMA((layers, len(PARTS), 2)),
            pltpu.SemaphoreType.DMA((layers, len(PARTS), 2)),
            pltpu.SemaphoreType.DMA((layers, C_PARTS)),
            pltpu.SemaphoreType.DMA((layers, C_PARTS)),
        ],
        compiler_params=pltpu.CompilerParams(
            collective_id=0, has_side_effects=True, vmem_limit_bytes=48 * 1024 * 1024
        ),
    )(*[pltpu.with_memory_space_constraint(a, pltpu.HBM) for a in (hidden, norm_gains, w_query, w_key, w_value, w_out, keys, values, lengths)])


def solution(mesh):
    finer = Mesh(mesh.devices.reshape(RING, RING, mesh.shape["tp"]), CTX + ("tp",))
    return jax.shard_map(
        on_device,
        mesh=finer,
        in_specs=(
            P(None, CTX),
            P(None, CTX),
            P(None, CTX, "tp"),
            P(None, CTX, "tp"),
            P(None, CTX, "tp"),
            P(None, "tp", CTX),
            P(None, None, "tp", CTX, None),
            P(None, None, "tp", CTX, None),
            P(),
        ),
        out_specs=P(None, CTX),
        check_vma=False,
    )
```

```python
import functools
import math

import jax
import jax.numpy as jnp
from jax import lax
from jax.experimental import pallas as pl
from jax.experimental.pallas import tpu as pltpu
from jax.sharding import Mesh
from jax.sharding import PartitionSpec as P

CTX = ("ctx_0", "ctx_1")
MESH = pl.DeviceIdType.MESH
NORM_EPS = 1e-05
ROPE_BASE = 500000.0
MASK_FILL = -1e30
RING = 4
FAR_FIRST = (2, 1, 3, 0)
TP_STEPS = ((2, 0), (2, 1), (1, 0), (1, 1), (3, 0), (3, 1), (0, 1))
A_PARTS = ((False, (0, 1), 1), (True, (2, 3, 4), 0), (False, (5, 6, 7), 0), (True, (8, 9), 0))
B_PARTS = ((False, (0, 1), 1), (True, (4, 5), 1), (False, (2, 3), 0), (True, (6, 7), 0))
PARTS = A_PARTS + B_PARTS
C_PARTS = 1


def kernel(
    layers, batch, heads, width, span, features,
    hidden_hbm, gains_hbm, wq_hbm, wk_hbm, wv_hbm, wo_hbm, kc_hbm, vc_hbm, lengths_hbm,
    out_ref,
    lengths, hidden_v, gains_v, wqkv, wo, kcat, vcat, turned, diag,
    *rest,
):
    y = lax.axis_index("ctx_0")
    x = lax.axis_index("ctx_1")
    tp = lax.axis_index("tp")
    z, core = tp // 2, lax.rem(tp, 2)
    n = len(PARTS)
    arrived, sent, (cbuf, in_sem, w_sem, wq_sem, p_send, p_recv, c_send, c_recv) = rest[:2 * n], rest[2 * n:4 * n], rest[4 * n:]
    columns = heads * width
    f32, bf16 = jnp.float32, jnp.bfloat16

    def tp_partner(step, sign=1):
        dz, other = step
        zz = lax.rem(z + (dz if sign > 0 else RING - dz), RING)
        cc = 1 - core if other else core
        return zz * 2 + cc

    barrier = pltpu.get_barrier_semaphore()
    swapped = tp + 1 - 2 * core
    for d in FAR_FIRST[:-1]:
        pl.semaphore_signal(
            barrier, inc=1, device_id={"ctx_1": lax.rem(x + d, RING), "tp": swapped}, device_id_type=MESH
        )
        pl.semaphore_signal(
            barrier, inc=1, device_id={"ctx_0": lax.rem(y + d, RING), "tp": swapped}, device_id_type=MESH
        )
    for step in TP_STEPS:
        pl.semaphore_signal(barrier, inc=1, device_id={"tp": tp_partner(step)}, device_id_type=MESH)

    def weight_copies(l):
        copies = []
        for p, (_, hs, _) in enumerate(A_PARTS[:-1]):
            at = pl.ds(hs[0] * width, len(hs) * width)
            copies.append(pltpu.make_async_copy(wq_hbm.at[l, :, at], wqkv.at[l, :, at], wq_sem.at[l, p]))
        return copies + [
            pltpu.make_async_copy(wk_hbm.at[l], wqkv.at[l, :, pl.ds(columns, width)], w_sem.at[l, 1]),
            pltpu.make_async_copy(wv_hbm.at[l], wqkv.at[l, :, pl.ds(columns + width, width)], w_sem.at[l, 2]),
        ]

    def late_start(l):
        for b in range(batch):
            pltpu.make_async_copy(
                kc_hbm.at[l, b], kcat.at[l, :, pl.ds(b * width, width)], w_sem.at[l, 3]
            ).start()
        pltpu.make_async_copy(vc_hbm.at[l], vcat.at[l], w_sem.at[l, 4]).start()
        pltpu.make_async_copy(wo_hbm.at[l], wo.at[l], w_sem.at[l, 5]).start()

    hidden_copy = pltpu.make_async_copy(hidden_hbm, hidden_v, in_sem.at[0])
    gains_copy = pltpu.make_async_copy(gains_hbm, gains_v, in_sem.at[1])
    lengths_copy = pltpu.make_async_copy(lengths_hbm, lengths, in_sem.at[2])
    hidden_copy.start()
    gains_copy.start()
    for copy in weight_copies(0):
        copy.start()
    lengths_copy.start()

    lengths_copy.wait()
    row = lax.broadcasted_iota(jnp.int32, (batch, width), 0)
    lane = lax.broadcasted_iota(jnp.int32, (batch, width), 1)
    half = width // 2
    length = jnp.zeros((batch, width), jnp.int32)
    for b in range(batch):
        length = jnp.where(row == b, lengths[b], length)
    low = lane < half
    exponents = jnp.where(low, lane, lane - half).astype(f32) * (2.0 / width)
    angles = length.astype(f32) * jnp.exp(-exponents * math.log(ROPE_BASE))
    cosine = jnp.cos(angles)
    sine = jnp.where(low, -jnp.sin(angles), jnp.sin(angles))
    usable = (y * RING + x) * span + lane < length
    scale = 1.0 / math.sqrt(width)
    wide_row = lax.broadcasted_iota(jnp.int32, (2 * batch, batch * width), 0)
    wide_col = lax.broadcasted_iota(jnp.int32, (2 * batch, batch * width), 1)
    own_block = jnp.where(lax.rem(wide_row, batch) == wide_col // width, 1.0, 0.0).astype(bf16)
    for part in range(heads // 2):
        diag[pl.ds(part * 2 * batch, 2 * batch), :] = own_block

    def spread(tall):
        return jnp.concatenate([tall] * batch, axis=1) * diag[...]

    def start(l, p, e):
        axis, me = ("ctx_1", x) if PARTS[p][0] == (e == 0) else ("ctx_0", y)
        for d in FAR_FIRST:
            pltpu.make_async_remote_copy(
                src_ref=sent[2 * p + e].at[l], dst_ref=arrived[2 * p + e].at[l, me],
                send_sem=p_send.at[l, p, e], recv_sem=p_recv.at[l, p, e],
                device_id={axis: lax.rem(me + d, RING), "tp": swapped}, device_id_type=MESH,
            ).start()

    def bytes_of(ref, sem):
        pltpu.make_async_copy(ref, ref, sem).wait()

    def arrive(l, p, e):
        bytes_of(arrived[2 * p + e].at[l], p_recv.at[l, p, e])

    def all_sent(l, parts):
        for p in parts:
            for e in range(2):
                bytes_of(arrived[2 * p + e].at[l], p_send.at[l, p, e])

    def tp_start(l, part):
        partners = [lax.rem(z + dz, RING) * 2 + to for dz in (2, 1, 3) for to in (0, 1)] + [swapped]
        for partner in partners:
            pltpu.make_async_remote_copy(
                src_ref=cbuf.at[l, part, tp], dst_ref=cbuf.at[l, part, tp],
                send_sem=c_send.at[l, part], recv_sem=c_recv.at[l, part],
                device_id={"tp": partner}, device_id_type=MESH,
            ).start()

    def total(l, p, e):
        buf = arrived[2 * p + e]
        return (buf[l, 0] + buf[l, 1]) + (buf[l, 2] + buf[l, 3])

    def tile(values, i):
        return values[:, i * width:(i + 1) * width]

    def over_lane(values, i):
        return jnp.broadcast_to(values[:, i:i + 1], (batch, width))

    def weighted(l, p, e, factors):
        buf = arrived[2 * p + e]
        out = []
        for k, h in enumerate(PARTS[p][1]):
            terms = [
                over_lane(factors[s], h % (heads // 2)) * buf[l, s, :, pl.ds(k * width, width)]
                for s in range(RING)
            ]
            out.append((terms[0] + terms[1]) + (terms[2] + terms[3]))
        return out

    def stats_of(l, p, e):
        at = len(PARTS[p][1]) * width
        return [arrived[2 * p + e][l, s, :, pl.ds(at, width)] for s in range(RING)]

    def put(l, p, e, tiles):
        for k, t in enumerate(tiles):
            sent[2 * p + e][l, :, pl.ds(k * width, width)] = t

    hidden_copy.wait()
    gains_copy.wait()

    def layer(l, stream):
        copies = weight_copies(l)
        if l > 0:
            for copy in copies:
                copy.wait()
        gain = gains_v[pl.ds(l, 1), :].astype(f32)
        scaled = (stream * gain).astype(bf16)
        squares = stream * stream
        squares = functools.reduce(jnp.add, [tile(squares, i) for i in range(features // width)])
        products = []
        for p, (_, hs, _) in enumerate(A_PARTS):
            if l == 0:
                for copy in copies[p:p + 1] if p < len(A_PARTS) - 1 else copies[p:]:
                    copy.wait()
            products.append(
                jnp.dot(scaled, wqkv[l, :, pl.ds(hs[0] * width, len(hs) * width)], preferred_element_type=f32)
            )
        a_ids, b_ids = range(len(A_PARTS)), range(len(A_PARTS), n)
        for p in a_ids:
            sent[2 * p][l, :, pl.ds(0, len(PARTS[p][1]) * width)] = products[p]
            if PARTS[p][2]:
                sent[2 * p][l, :, pl.ds(2 * width, width)] = squares
            if l == 0 and p == 0:
                pl.semaphore_wait(barrier, 2 * (RING - 1) + len(TP_STEPS))
            start(l, p, 0)
        if l == 0:
            late_start(0)
        for p in a_ids:
            arrive(l, p, 0)
            sent[2 * p + 1][l] = total(l, p, 0)
            start(l, p, 1)
        if l + 1 < layers:
            for copy in weight_copies(l + 1):
                copy.start()
        bytes_of(kcat.at[l], w_sem.at[l, 3])
        turned[...] = kcat[l].T

        query = [None] * heads
        for p in a_ids[:-1]:
            arrive(l, p, 1)
            raw = total(l, p, 1)
            if PARTS[p][2]:
                mean = jnp.sum(tile(raw, 2), axis=1, keepdims=True) / (RING * RING * features)
                inverse = jnp.broadcast_to(lax.rsqrt(mean + NORM_EPS), (batch, width))
                turn_cos, turn_sin = cosine * inverse, sine * inverse
            for k, h in enumerate(PARTS[p][1]):
                u = tile(raw, k)
                query[h] = (u * turn_cos + pltpu.roll(u, half, axis=1) * turn_sin).astype(bf16)
        tall = jnp.concatenate(query, axis=0)
        scores = lax.dot_general(
            spread(tall), turned[...], (((1,), (0,)), ((), ())), preferred_element_type=f32
        ) * scale
        group = heads // 2
        stats = [jnp.zeros((batch, width), f32)] * 2
        weights = []
        for h in range(heads):
            masked = jnp.where(usable, scores[h * batch:(h + 1) * batch], MASK_FILL)
            top = jnp.max(masked, axis=1, keepdims=True)
            weight = jnp.where(usable, jnp.exp(masked - top), 0.0)
            amount = jnp.sum(weight, axis=1, keepdims=True)
            weights.append(weight.astype(bf16))
            i = h % group
            stats[h // group] = jnp.where(
                lane == i, top, jnp.where(lane == half + i, amount, stats[h // group])
            )
        bytes_of(vcat.at[l], w_sem.at[l, 4])
        sums = jnp.dot(
            spread(jnp.concatenate(weights, axis=0)), vcat[l], preferred_element_type=f32
        )
        for p in b_ids:
            _, hs, more = PARTS[p]
            put(l, p, 0, [sums[h * batch:(h + 1) * batch] for h in hs] + [stats[hs[0] // group]] * more)
            start(l, p, 0)

        if l + 1 < layers:
            late_start(l + 1)

        p = a_ids[-1]
        arrive(l, p, 1)
        raw = total(l, p, 1)
        u = tile(raw, 0)
        new_key = (u * turn_cos + pltpu.roll(u, half, axis=1) * turn_sin).astype(bf16).astype(f32)
        new_value = (tile(raw, 1) * inverse).astype(bf16).astype(f32)
        own = []
        for g in range(2):
            packed = jnp.where(lane >= half, 1.0, 0.0)
            for i in range(group):
                match = jnp.sum(query[g * group + i].astype(f32) * new_key, axis=1, keepdims=True)
                packed = jnp.where(lane == i, match * scale, packed)
            own.append(packed)
        all_sent(l, a_ids)
        bytes_of(wo.at[l], w_sem.at[l, 5])

        shrink = [None, None]
        for p in b_ids:
            arrive(l, p, 0)
            _, hs, more = PARTS[p]
            g = hs[0] // group
            tiles = []
            if more:
                each = stats_of(l, p, 0)
                top = functools.reduce(jnp.maximum, each)
                shrink[g] = [jnp.exp(t - top) for t in each]
                amount = functools.reduce(
                    jnp.add, [pltpu.roll(e, half, axis=1) * t for e, t in zip(shrink[g], each)]
                )
                tiles = [jnp.where(low, top, amount)]
            put(l, p, 1, weighted(l, p, 0, shrink[g]) + tiles)
            start(l, p, 1)

        share = [None, None]
        out = [None] * C_PARTS
        piece = features // C_PARTS
        for p in b_ids:
            arrive(l, p, 1)
            _, hs, more = PARTS[p]
            g = hs[0] // group
            if more:
                each = stats_of(l, p, 1) + [own[g]]
                top = functools.reduce(jnp.maximum, each)
                factors = [jnp.exp(t - top) for t in each]
                amount = functools.reduce(
                    jnp.add, [e * pltpu.roll(t, half, axis=1) for e, t in zip(factors, each)]
                )
                share[g] = [e / amount for e in factors]
            context = [
                v + over_lane(share[g][RING], h % group) * new_value
                for v, h in zip(weighted(l, p, 1, share[g]), hs)
            ]
            context = jnp.concatenate(context, axis=1).astype(bf16)
            for c in range(C_PARTS):
                product = jnp.dot(
                    context, wo[l, pl.ds(hs[0] * width, len(hs) * width), pl.ds(c * piece, piece)],
                    preferred_element_type=f32,
                )
                out[c] = product if out[c] is None else out[c] + product
        for c in range(C_PARTS):
            cbuf[l, c, tp] = out[c]
            tp_start(l, c)
        all_sent(l, b_ids)
        pieces = []
        for c in range(C_PARTS):
            bytes_of(cbuf.at[l, c, pl.ds(0, len(TP_STEPS))], c_recv.at[l, c])
            t = [cbuf[l, c, i] for i in range(2 * RING)]
            pieces.append(((t[0] + t[1]) + (t[2] + t[3])) + ((t[4] + t[5]) + (t[6] + t[7])))
        stream = stream + jnp.concatenate(pieces, axis=1)
        for c in range(C_PARTS):
            bytes_of(cbuf.at[l, c, pl.ds(0, len(TP_STEPS))], c_send.at[l, c])
        return stream

    stream = hidden_v[...].astype(f32)
    for l in range(layers):
        stream = layer(l, stream)
    out_ref[...] = stream


def on_device(hidden, norm_gains, w_query, w_key, w_value, w_out, key_cache, value_cache, lengths):
    layers, features, columns = w_query.shape
    batch, _, span, width = key_cache.shape[1:]
    heads = columns // width
    keys = key_cache.reshape(layers, batch, span, width)
    values = value_cache.reshape(layers, batch * span, width)
    f32, bf16 = jnp.float32, jnp.bfloat16
    messages = [(len(hs) + more) * width for _, hs, more in PARTS for _ in range(2)]
    return pl.pallas_call(
        functools.partial(kernel, layers, batch, heads, width, span, features),
        out_shape=jax.ShapeDtypeStruct((batch, features), f32),
        in_specs=[pl.BlockSpec(memory_space=pltpu.HBM)] * 9,
        out_specs=pl.BlockSpec(memory_space=pltpu.VMEM),
        scratch_shapes=[
            pltpu.SMEM((batch,), jnp.int32),
            pltpu.VMEM((batch, features), bf16),
            pltpu.VMEM((layers, features), bf16),
            pltpu.VMEM((layers, features, columns + 2 * width), bf16),
            pltpu.VMEM((layers, columns, features), bf16),
            pltpu.VMEM((layers, span, batch * width), bf16),
            pltpu.VMEM((layers, batch * span, width), bf16),
            pltpu.VMEM((batch * width, span), bf16),
            pltpu.VMEM((heads * batch, batch * width), bf16),
            *[pltpu.VMEM((layers, RING, batch, w), f32) for w in messages],
            *[pltpu.VMEM((layers, batch, w), f32) for w in messages],
            pltpu.VMEM((layers, C_PARTS, 2 * RING, batch, features // C_PARTS), f32),
            pltpu.SemaphoreType.DMA((3,)),
            pltpu.SemaphoreType.DMA((layers, 6)),
            pltpu.SemaphoreType.DMA((layers, len(A_PARTS) - 1)),
            pltpu.SemaphoreType.DMA((layers, len(PARTS), 2)),
            pltpu.SemaphoreType.DMA((layers, len(PARTS), 2)),
            pltpu.SemaphoreType.DMA((layers, C_PARTS)),
            pltpu.SemaphoreType.DMA((layers, C_PARTS)),
        ],
        compiler_params=pltpu.CompilerParams(
            collective_id=0, has_side_effects=True, vmem_limit_bytes=48 * 1024 * 1024
        ),
    )(*[pltpu.with_memory_space_constraint(a, pltpu.HBM) for a in (hidden, norm_gains, w_query, w_key, w_value, w_out, keys, values, lengths)])


def solution(mesh):
    finer = Mesh(mesh.devices.reshape(RING, RING, mesh.shape["tp"]), CTX + ("tp",))
    return jax.shard_map(
        on_device,
        mesh=finer,
        in_specs=(
            P(None, CTX),
            P(None, CTX),
            P(None, CTX, "tp"),
            P(None, CTX, "tp"),
            P(None, CTX, "tp"),
            P(None, "tp", CTX),
            P(None, None, "tp", CTX, None),
            P(None, None, "tp", CTX, None),
            P(),
        ),
        out_specs=P(None, CTX),
        check_vma=False,
    )
```

```python
import functools
import math

import jax
import jax.numpy as jnp
from jax import lax
from jax.experimental import pallas as pl
from jax.experimental.pallas import tpu as pltpu
from jax.sharding import Mesh
from jax.sharding import PartitionSpec as P

CTX = ("ctx_0", "ctx_1")
MESH = pl.DeviceIdType.MESH
NORM_EPS = 1e-05
ROPE_BASE = 500000.0
MASK_FILL = -1e30
RING = 4
FAR_FIRST = (2, 1, 3, 0)
TP_STEPS = ((2, 0), (2, 1), (1, 0), (1, 1), (3, 0), (3, 1), (0, 1))
A_PARTS = ((False, (0, 1), 1), (True, (2, 3, 4), 0), (False, (5, 6, 7), 0), (True, (8, 9), 0))
B_PARTS = ((False, (0, 1), 1), (True, (4, 5), 1), (False, (2, 3), 0), (True, (6, 7), 0))
PARTS = A_PARTS + B_PARTS
C_PARTS = 1


def kernel(
    layers, batch, heads, width, span, features,
    hidden_hbm, gains_hbm, wq_hbm, wk_hbm, wv_hbm, wo_hbm, kc_hbm, vc_hbm, lengths_hbm,
    out_ref,
    lengths, hidden_v, gains_v, wqkv, wo, kcat, vcat, turned, diag,
    *rest,
):
    y = lax.axis_index("ctx_0")
    x = lax.axis_index("ctx_1")
    tp = lax.axis_index("tp")
    z, core = tp // 2, lax.rem(tp, 2)
    n = len(PARTS)
    arrived, sent, (cbuf, in_sem, w_sem, wq_sem, p_send, p_recv, c_send, c_recv) = rest[:2 * n], rest[2 * n:4 * n], rest[4 * n:]
    columns = heads * width
    f32, bf16 = jnp.float32, jnp.bfloat16

    def tp_partner(step, sign=1):
        dz, other = step
        zz = lax.rem(z + (dz if sign > 0 else RING - dz), RING)
        cc = 1 - core if other else core
        return zz * 2 + cc

    barrier = pltpu.get_barrier_semaphore()
    swapped = tp + 1 - 2 * core
    for d in FAR_FIRST[:-1]:
        pl.semaphore_signal(
            barrier, inc=1, device_id={"ctx_1": lax.rem(x + d, RING), "tp": swapped}, device_id_type=MESH
        )
        pl.semaphore_signal(
            barrier, inc=1, device_id={"ctx_0": lax.rem(y + d, RING), "tp": swapped}, device_id_type=MESH
        )
    for step in TP_STEPS:
        pl.semaphore_signal(barrier, inc=1, device_id={"tp": tp_partner(step)}, device_id_type=MESH)

    def weight_copies(l):
        copies = []
        for p, (_, hs, _) in enumerate(A_PARTS[:-1]):
            at = pl.ds(hs[0] * width, len(hs) * width)
            copies.append(pltpu.make_async_copy(wq_hbm.at[l, :, at], wqkv.at[l, :, at], wq_sem.at[l, p]))
        return copies + [
            pltpu.make_async_copy(wk_hbm.at[l], wqkv.at[l, :, pl.ds(columns, width)], w_sem.at[l, 1]),
            pltpu.make_async_copy(wv_hbm.at[l], wqkv.at[l, :, pl.ds(columns + width, width)], w_sem.at[l, 2]),
        ]

    def late_start(l):
        for b in range(batch):
            pltpu.make_async_copy(
                kc_hbm.at[l, b], kcat.at[l, :, pl.ds(b * width, width)], w_sem.at[l, 3]
            ).start()
        pltpu.make_async_copy(vc_hbm.at[l], vcat.at[l], w_sem.at[l, 4]).start()
        pltpu.make_async_copy(wo_hbm.at[l], wo.at[l], w_sem.at[l, 5]).start()

    hidden_copy = pltpu.make_async_copy(hidden_hbm, hidden_v, in_sem.at[0])
    gains_copy = pltpu.make_async_copy(gains_hbm, gains_v, in_sem.at[1])
    lengths_copy = pltpu.make_async_copy(lengths_hbm, lengths, in_sem.at[2])
    hidden_copy.start()
    gains_copy.start()
    for copy in weight_copies(0):
        copy.start()
    lengths_copy.start()

    lengths_copy.wait()
    row = lax.broadcasted_iota(jnp.int32, (batch, width), 0)
    lane = lax.broadcasted_iota(jnp.int32, (batch, width), 1)
    half = width // 2
    length = jnp.zeros((batch, width), jnp.int32)
    for b in range(batch):
        length = jnp.where(row == b, lengths[b], length)
    low = lane < half
    exponents = jnp.where(low, lane, lane - half).astype(f32) * (2.0 / width)
    angles = length.astype(f32) * jnp.exp(-exponents * math.log(ROPE_BASE))
    cosine = jnp.cos(angles)
    sine = jnp.where(low, -jnp.sin(angles), jnp.sin(angles))
    usable = (y * RING + x) * span + lane < length
    scale = 1.0 / math.sqrt(width)
    wide_row = lax.broadcasted_iota(jnp.int32, (2 * batch, batch * width), 0)
    wide_col = lax.broadcasted_iota(jnp.int32, (2 * batch, batch * width), 1)
    own_block = jnp.where(lax.rem(wide_row, batch) == wide_col // width, 1.0, 0.0).astype(bf16)
    for part in range(heads // 2):
        diag[pl.ds(part * 2 * batch, 2 * batch), :] = own_block

    def spread(tall):
        return jnp.concatenate([tall] * batch, axis=1) * diag[...]

    def start(l, p, e):
        axis, me = ("ctx_1", x) if PARTS[p][0] == (e == 0) else ("ctx_0", y)
        for d in FAR_FIRST:
            pltpu.make_async_remote_copy(
                src_ref=sent[2 * p + e].at[l], dst_ref=arrived[2 * p + e].at[l, me],
                send_sem=p_send.at[l, p, e], recv_sem=p_recv.at[l, p, e],
                device_id={axis: lax.rem(me + d, RING), "tp": swapped}, device_id_type=MESH,
            ).start()

    def bytes_of(ref, sem):
        pltpu.make_async_copy(ref, ref, sem).wait()

    def arrive(l, p, e):
        bytes_of(arrived[2 * p + e].at[l], p_recv.at[l, p, e])

    def all_sent(l, parts):
        for p in parts:
            for e in range(2):
                bytes_of(arrived[2 * p + e].at[l], p_send.at[l, p, e])

    def tp_start(l, part):
        partners = [lax.rem(z + dz, RING) * 2 + to for dz in (2, 1, 3) for to in (0, 1)] + [swapped]
        for partner in partners:
            pltpu.make_async_remote_copy(
                src_ref=cbuf.at[l, part, tp], dst_ref=cbuf.at[l, part, tp],
                send_sem=c_send.at[l, part], recv_sem=c_recv.at[l, part],
                device_id={"tp": partner}, device_id_type=MESH,
            ).start()

    def total(l, p, e):
        buf = arrived[2 * p + e]
        return (buf[l, 0] + buf[l, 1]) + (buf[l, 2] + buf[l, 3])

    def tile(values, i):
        return values[:, i * width:(i + 1) * width]

    def over_lane(values, i):
        return jnp.broadcast_to(values[:, i:i + 1], (batch, width))

    def weighted(l, p, e, factors):
        buf = arrived[2 * p + e]
        out = []
        for k, h in enumerate(PARTS[p][1]):
            terms = [
                over_lane(factors[s], h % (heads // 2)) * buf[l, s, :, pl.ds(k * width, width)]
                for s in range(RING)
            ]
            out.append((terms[0] + terms[1]) + (terms[2] + terms[3]))
        return out

    def stats_of(l, p, e):
        at = len(PARTS[p][1]) * width
        return [arrived[2 * p + e][l, s, :, pl.ds(at, width)] for s in range(RING)]

    def put(l, p, e, tiles):
        for k, t in enumerate(tiles):
            sent[2 * p + e][l, :, pl.ds(k * width, width)] = t

    hidden_copy.wait()
    gains_copy.wait()

    def layer(l, stream):
        copies = weight_copies(l)
        if l > 0:
            for copy in copies:
                copy.wait()
        gain = gains_v[pl.ds(l, 1), :].astype(f32)
        scaled = (stream * gain).astype(bf16)
        squares = stream * stream
        squares = functools.reduce(jnp.add, [tile(squares, i) for i in range(features // width)])
        products = []
        for p, (_, hs, _) in enumerate(A_PARTS):
            if l == 0:
                for copy in copies[p:p + 1] if p < len(A_PARTS) - 1 else copies[p:]:
                    copy.wait()
            products.append(
                jnp.dot(scaled, wqkv[l, :, pl.ds(hs[0] * width, len(hs) * width)], preferred_element_type=f32)
            )
        a_ids, b_ids = range(len(A_PARTS)), range(len(A_PARTS), n)
        for p in a_ids:
            sent[2 * p][l, :, pl.ds(0, len(PARTS[p][1]) * width)] = products[p]
            if PARTS[p][2]:
                sent[2 * p][l, :, pl.ds(2 * width, width)] = squares
            if l == 0 and p == 0:
                pl.semaphore_wait(barrier, 2 * (RING - 1) + len(TP_STEPS))
            start(l, p, 0)
        if l == 0:
            late_start(0)
        for p in a_ids:
            arrive(l, p, 0)
            sent[2 * p + 1][l] = total(l, p, 0)
            start(l, p, 1)
        if l + 1 < layers:
            for copy in weight_copies(l + 1):
                copy.start()
        bytes_of(kcat.at[l], w_sem.at[l, 3])
        turned[...] = kcat[l].T

        query = [None] * heads
        for p in a_ids[:-1]:
            arrive(l, p, 1)
            raw = total(l, p, 1)
            if PARTS[p][2]:
                mean = jnp.sum(tile(raw, 2), axis=1, keepdims=True) / (RING * RING * features)
                inverse = jnp.broadcast_to(lax.rsqrt(mean + NORM_EPS), (batch, width))
                turn_cos, turn_sin = cosine * inverse, sine * inverse
            for k, h in enumerate(PARTS[p][1]):
                u = tile(raw, k)
                query[h] = (u * turn_cos + pltpu.roll(u, half, axis=1) * turn_sin).astype(bf16)
        tall = jnp.concatenate(query, axis=0)
        scores = lax.dot_general(
            spread(tall), turned[...], (((1,), (0,)), ((), ())), preferred_element_type=f32
        ) * scale
        group = heads // 2
        stats = [jnp.zeros((batch, width), f32)] * 2
        weights = []
        for h in range(heads):
            masked = jnp.where(usable, scores[h * batch:(h + 1) * batch], MASK_FILL)
            top = jnp.maximum(jnp.max(masked, axis=1, keepdims=True), 0.1 * MASK_FILL)
            weight = jnp.exp(masked - top)
            amount = jnp.sum(weight, axis=1, keepdims=True)
            weights.append(weight.astype(bf16))
            i = h % group
            stats[h // group] = jnp.where(
                lane == i, top, jnp.where(lane == half + i, amount, stats[h // group])
            )
        bytes_of(vcat.at[l], w_sem.at[l, 4])
        sums = jnp.dot(
            spread(jnp.concatenate(weights, axis=0)), vcat[l], preferred_element_type=f32
        )
        for p in b_ids:
            _, hs, more = PARTS[p]
            put(l, p, 0, [sums[h * batch:(h + 1) * batch] for h in hs] + [stats[hs[0] // group]] * more)
            start(l, p, 0)

        if l + 1 < layers:
            late_start(l + 1)

        p = a_ids[-1]
        arrive(l, p, 1)
        raw = total(l, p, 1)
        u = tile(raw, 0)
        new_key = (u * turn_cos + pltpu.roll(u, half, axis=1) * turn_sin).astype(bf16).astype(f32)
        new_value = (tile(raw, 1) * inverse).astype(bf16).astype(f32)
        own = []
        for g in range(2):
            packed = jnp.where(lane >= half, 1.0, 0.0)
            for i in range(group):
                match = jnp.sum(query[g * group + i].astype(f32) * new_key, axis=1, keepdims=True)
                packed = jnp.where(lane == i, match * scale, packed)
            own.append(packed)
        all_sent(l, a_ids)
        bytes_of(wo.at[l], w_sem.at[l, 5])

        shrink = [None, None]
        for p in b_ids:
            arrive(l, p, 0)
            _, hs, more = PARTS[p]
            g = hs[0] // group
            tiles = []
            if more:
                each = stats_of(l, p, 0)
                top = functools.reduce(jnp.maximum, each)
                shrink[g] = [jnp.exp(t - top) for t in each]
                amount = functools.reduce(
                    jnp.add, [pltpu.roll(e, half, axis=1) * t for e, t in zip(shrink[g], each)]
                )
                tiles = [jnp.where(low, top, amount)]
            put(l, p, 1, weighted(l, p, 0, shrink[g]) + tiles)
            start(l, p, 1)

        share = [None, None]
        out = [None] * C_PARTS
        piece = features // C_PARTS
        for p in b_ids:
            arrive(l, p, 1)
            _, hs, more = PARTS[p]
            g = hs[0] // group
            if more:
                each = stats_of(l, p, 1) + [own[g]]
                top = functools.reduce(jnp.maximum, each)
                factors = [jnp.exp(t - top) for t in each]
                amount = functools.reduce(
                    jnp.add, [e * pltpu.roll(t, half, axis=1) for e, t in zip(factors, each)]
                )
                share[g] = [e / amount for e in factors]
            context = [
                v + over_lane(share[g][RING], h % group) * new_value
                for v, h in zip(weighted(l, p, 1, share[g]), hs)
            ]
            context = jnp.concatenate(context, axis=1).astype(bf16)
            for c in range(C_PARTS):
                product = jnp.dot(
                    context, wo[l, pl.ds(hs[0] * width, len(hs) * width), pl.ds(c * piece, piece)],
                    preferred_element_type=f32,
                )
                out[c] = product if out[c] is None else out[c] + product
        for c in range(C_PARTS):
            cbuf[l, c, tp] = out[c]
            tp_start(l, c)
        all_sent(l, b_ids)
        pieces = []
        for c in range(C_PARTS):
            bytes_of(cbuf.at[l, c, pl.ds(0, len(TP_STEPS))], c_recv.at[l, c])
            t = [cbuf[l, c, i] for i in range(2 * RING)]
            pieces.append(((t[0] + t[1]) + (t[2] + t[3])) + ((t[4] + t[5]) + (t[6] + t[7])))
        stream = stream + jnp.concatenate(pieces, axis=1)
        for c in range(C_PARTS):
            bytes_of(cbuf.at[l, c, pl.ds(0, len(TP_STEPS))], c_send.at[l, c])
        return stream

    stream = hidden_v[...].astype(f32)
    for l in range(layers):
        stream = layer(l, stream)
    out_ref[...] = stream


def on_device(hidden, norm_gains, w_query, w_key, w_value, w_out, key_cache, value_cache, lengths):
    layers, features, columns = w_query.shape
    batch, _, span, width = key_cache.shape[1:]
    heads = columns // width
    keys = key_cache.reshape(layers, batch, span, width)
    values = value_cache.reshape(layers, batch * span, width)
    f32, bf16 = jnp.float32, jnp.bfloat16
    messages = [(len(hs) + more) * width for _, hs, more in PARTS for _ in range(2)]
    return pl.pallas_call(
        functools.partial(kernel, layers, batch, heads, width, span, features),
        out_shape=jax.ShapeDtypeStruct((batch, features), f32),
        in_specs=[pl.BlockSpec(memory_space=pltpu.HBM)] * 9,
        out_specs=pl.BlockSpec(memory_space=pltpu.VMEM),
        scratch_shapes=[
            pltpu.SMEM((batch,), jnp.int32),
            pltpu.VMEM((batch, features), bf16),
            pltpu.VMEM((layers, features), bf16),
            pltpu.VMEM((layers, features, columns + 2 * width), bf16),
            pltpu.VMEM((layers, columns, features), bf16),
            pltpu.VMEM((layers, span, batch * width), bf16),
            pltpu.VMEM((layers, batch * span, width), bf16),
            pltpu.VMEM((batch * width, span), bf16),
            pltpu.VMEM((heads * batch, batch * width), bf16),
            *[pltpu.VMEM((layers, RING, batch, w), f32) for w in messages],
            *[pltpu.VMEM((layers, batch, w), f32) for w in messages],
            pltpu.VMEM((layers, C_PARTS, 2 * RING, batch, features // C_PARTS), f32),
            pltpu.SemaphoreType.DMA((3,)),
            pltpu.SemaphoreType.DMA((layers, 6)),
            pltpu.SemaphoreType.DMA((layers, len(A_PARTS) - 1)),
            pltpu.SemaphoreType.DMA((layers, len(PARTS), 2)),
            pltpu.SemaphoreType.DMA((layers, len(PARTS), 2)),
            pltpu.SemaphoreType.DMA((layers, C_PARTS)),
            pltpu.SemaphoreType.DMA((layers, C_PARTS)),
        ],
        compiler_params=pltpu.CompilerParams(
            collective_id=0, has_side_effects=True, vmem_limit_bytes=48 * 1024 * 1024
        ),
    )(*[pltpu.with_memory_space_constraint(a, pltpu.HBM) for a in (hidden, norm_gains, w_query, w_key, w_value, w_out, keys, values, lengths)])


def solution(mesh):
    finer = Mesh(mesh.devices.reshape(RING, RING, mesh.shape["tp"]), CTX + ("tp",))
    return jax.shard_map(
        on_device,
        mesh=finer,
        in_specs=(
            P(None, CTX),
            P(None, CTX),
            P(None, CTX, "tp"),
            P(None, CTX, "tp"),
            P(None, CTX, "tp"),
            P(None, "tp", CTX),
            P(None, None, "tp", CTX, None),
            P(None, None, "tp", CTX, None),
            P(),
        ),
        out_specs=P(None, CTX),
        check_vma=False,
    )
```
